64 devices in a mesh: rep: 4 (over x, y), dp: 16 (over z, core).
Axes of the slice: x: 2, y: 2, z: 8, core: 2. Of those that a mesh axis runs over, the one named last changes fastest.
The devices are a block of a 4x4x8 slice.
Arguments:
- g_w_gate: bfloat16 [64, 2, 1024, 2816], P(('rep', 'dp')), parts along dimension 0
- g_w_up: bfloat16 [64, 2, 1024, 2816], P(('rep', 'dp')), parts along dimension 0
- g_w_down: bfloat16 [64, 2, 2816, 1024], P(('rep', 'dp')), parts along dimension 0
- w_gate: bfloat16 [2, 1024, 2816], replicated
- w_up: bfloat16 [2, 1024, 2816], replicated
- w_down: bfloat16 [2, 2816, 1024], replicated
- m_w_gate: float32 [2, 1024, 2816], P(None, 'dp')
- m_w_up: float32 [2, 1024, 2816], P(None, 'dp')
- m_w_down: float32 [2, 2816, 1024], P(None, 'dp')
- v_w_gate: float32 [2, 1024, 2816], P(None, 'dp')
- v_w_up: float32 [2, 1024, 2816], P(None, 'dp')
- v_w_down: float32 [2, 2816, 1024], P(None, 'dp')
Outputs:
- output 1: bfloat16 [8, 1024, 2816], P('rep'), parts along dimension 0
- output 2: bfloat16 [8, 1024, 2816], P('rep'), parts along dimension 0
- output 3: bfloat16 [8, 2816, 1024], P('rep'), parts along dimension 0
- output 4: float32 [8, 1024, 2816], P('rep', 'dp'), parts along dimension 0
- output 5: float32 [8, 1024, 2816], P('rep', 'dp'), parts along dimension 0
- output 6: float32 [8, 2816, 1024], P('rep', 'dp'), parts along dimension 0
- output 7: float32 [8, 1024, 2816], P('rep', 'dp'), parts along dimension 0
- output 8: float32 [8, 1024, 2816], P('rep', 'dp'), parts along dimension 0
- output 9: float32 [8, 2816, 1024], P('rep', 'dp'), parts along dimension 0
There are 4 independent parts. The reference program is written for one: setup_inputs(seed, part) draws one part's arguments, and reference() takes and returns one part's arrays. A program takes and returns all parts, laid end to end along the dimension named above; an argument that names none is the same for every part.
All inputs are finite; a program needn't handle non-finite values.
Results may differ from the reference program's by a relative error of at most 0.022.
Values are sent between devices in bfloat16 or wider.
A program may use at most 768 MiB of HBM per device.

```python
import jax
import jax.numpy as jnp
from jax import lax

DEVICES = 16
D = 1024
FF = 2816
LAYERS = 2
NAMES = ("w_gate", "w_up", "w_down")
SHAPES = {"w_gate": (LAYERS, D, FF), "w_up": (LAYERS, D, FF), "w_down": (LAYERS, FF, D)}


def setup_inputs(seed: int = 0, part: int = 0) -> dict:
    kz, *keys = jax.random.split(jax.random.key(seed), 1 + 5 * len(NAMES))
    loud = 2.0 ** jax.random.uniform(kz, (), jnp.float32, -1.0, 1.0)
    drawn = {}
    for name, key, both in zip(NAMES, keys[:3], keys[3:6], strict=True):
        own = jax.random.normal(jax.random.fold_in(key, part), (DEVICES, *SHAPES[name]), jnp.float32)
        shared = jax.random.normal(jax.random.fold_in(both, part), SHAPES[name], jnp.float32)
        drawn["g_" + name] = (loud * (0.7 * shared / DEVICES + 0.7 * own * DEVICES**-0.5)).astype(jnp.bfloat16)
    for name, key in zip(NAMES, keys[6:9], strict=True):
        drawn[name] = (jax.random.normal(key, SHAPES[name], jnp.float32) * SHAPES[name][1] ** -0.5).astype(jnp.bfloat16)
    for name, key in zip(NAMES, keys[9:12], strict=True):
        drawn["m_" + name] = loud * 0.5 * jax.random.normal(key, SHAPES[name], jnp.float32)
    for name, key in zip(NAMES, keys[12:15], strict=True):
        drawn["v_" + name] = loud * loud * jax.random.uniform(key, SHAPES[name], jnp.float32, 0.5, 1.5)
    return drawn


def adamw(w, m, v, g):
    m = 0.9 * m + 0.1 * g
    v = 0.95 * v + 0.05 * g * g
    step = m * lax.rsqrt(v + 1e-8) + 0.1 * w
    return (w - 0.02 * step).astype(jnp.bfloat16), m, v


def reference(g_w_gate, g_w_up, g_w_down, w_gate, w_up, w_down, m_w_gate, m_w_up, m_w_down, v_w_gate, v_w_up, v_w_down):
    def total(terms):
        return lax.scan(lambda so_far, term: (so_far + term.astype(jnp.float32), None), jnp.zeros(terms.shape[1:], jnp.float32), terms)[0]

    gradients = [total(terms).astype(jnp.bfloat16).astype(jnp.float32) for terms in (g_w_gate, g_w_up, g_w_down)]
    new = [
        adamw(w.astype(jnp.float32), m, v, g)
        for w, m, v, g in zip((w_gate, w_up, w_down), (m_w_gate, m_w_up, m_w_down), (v_w_gate, v_w_up, v_w_down), gradients, strict=True)
    ]
    return tuple(one[which] for which in range(3) for one in new)
```

```python
import functools

import jax
import jax.numpy as jnp
from jax import lax
from jax.experimental import pallas as pl
from jax.experimental.pallas import tpu as pltpu
from jax.sharding import PartitionSpec as P

CORES = 2
ROWS = 16
WAYS = 2


def adamw(w, m, v, g):
    m = 0.9 * m + 0.1 * g
    v = 0.95 * v + 0.05 * g * g
    step = m * lax.rsqrt(v + 1e-8) + 0.1 * w
    return (w - 0.02 * step).astype(jnp.bfloat16), m, v


def kernel(chips, count, *refs):
    def take(number):
        nonlocal refs
        head, refs = refs[:number], refs[number:]
        return head

    g, w, m, v = (take(count) for _ in range(4))
    w_out, m_out, v_out = (take(count) for _ in range(3))
    given, came, own, wb, mb, vb = (take(count) for _ in range(6))
    own_sem, give_send, give_recv, ring_send, ring_recv, in_sem, out_sem, ag_send, ag_recv, side_send, side_recv = refs

    me = lax.axis_index("dp")
    z, c = me // CORES, me % CORES
    other = 1 - c

    def chip(i):
        return (i + 2 * chips) % chips

    partner = {"dp": z * CORES + other}
    ahead = [{"dp": chip(z + 1) * CORES + c}, {"dp": chip(z - 1) * CORES + c}]
    parts = [(k, d) for k in range(count) for d in range(WAYS)]
    half = [one.shape[0] // WAYS for one in m]
    rows = [one.shape[1] for one in m]

    def block(k, d, chip_of, core):
        start = pl.multiple_of((chip_of * CORES + core) * rows[k], rows[k])
        return pl.ds(d * half[k], half[k]), pl.ds(start, rows[k])

    def turn(d, s):
        return chip(z - 1 - s) if d == 0 else chip(z + 1 + s)

    def load_own(s, k, d):
        layers, where = block(k, d, turn(d, s), c)
        return pltpu.make_async_copy(g[k].at[0, layers, where], own[k].at[s % 2, d], own_sem.at[s % 2, k, d])

    def give(s, k, d):
        layers, where = block(k, d, turn(d, s), other)
        return pltpu.make_async_remote_copy(
            g[k].at[0, layers, where], given[k].at[s, d], give_send.at[s, k, d], give_recv.at[s, k, d], device_id=partner
        )

    def ring(s, k, d):
        return pltpu.make_async_remote_copy(
            given[k].at[s, d], came[k].at[s, d], ring_send.at[s, k, d], ring_recv.at[s, k, d], device_id=ahead[d]
        )

    def load_state(k, d):
        layers, where = block(k, d, z, c)
        return [
            pltpu.make_async_copy(w[k].at[layers, where], wb[k].at[d], in_sem.at[0, k, d]),
            pltpu.make_async_copy(m[k].at[layers], mb[k].at[d], in_sem.at[1, k, d]),
            pltpu.make_async_copy(v[k].at[layers], vb[k].at[d], in_sem.at[2, k, d]),
        ]

    def store_state(k, d):
        layers, where = block(k, d, z, c)
        return [
            pltpu.make_async_copy(wb[k].at[d], w_out[k].at[layers, where], out_sem.at[0, k, d]),
            pltpu.make_async_copy(mb[k].at[d], m_out[k].at[layers], out_sem.at[1, k, d]),
            pltpu.make_async_copy(vb[k].at[d], v_out[k].at[layers], out_sem.at[2, k, d]),
        ]

    def gathered(t, k, d):
        layers, where = block(k, d, chip(z - t) if d == 0 else chip(z + t), c)
        return w_out[k].at[layers, where]

    def gather(t, k, d):
        here = gathered(t, k, d)
        return pltpu.make_async_remote_copy(
            wb[k].at[d] if isinstance(t, int) and t == 0 else here, here, ag_send.at[t, k, d], ag_recv.at[t, k, d], device_id=ahead[d]
        )

    def gather_recv(t, k, d):
        here = gathered(t + 1, k, d)
        return pltpu.make_async_remote_copy(here, here, ag_send.at[t, k, d], ag_recv.at[t, k, d], device_id=ahead[d])

    def side(t, k, d):
        here = gathered(t, k, d)
        return pltpu.make_async_remote_copy(
            wb[k].at[d] if isinstance(t, int) and t == 0 else here, here, side_send.at[t, k, d], side_recv.at[t, k, d], device_id=partner
        )

    def side_recv_of(t, k, d):
        layers, where = block(k, d, chip(z - t) if d == 0 else chip(z + t), other)
        here = w_out[k].at[layers, where]
        return pltpu.make_async_remote_copy(here, here, side_send.at[t, k, d], side_recv.at[t, k, d], device_id=partner)

    def by_rows(k, body):
        for h in range(half[k]):

            @pl.loop(0, rows[k] // ROWS)
            def _(i):
                body(h, pl.ds(pl.multiple_of(i * ROWS, ROWS), ROWS))

    def total(s, k, d, h, at, first):
        so_far = own[k][s % 2, d, h, at].astype(jnp.float32) + given[k][s, d, h, at].astype(jnp.float32)
        if not first:
            so_far = so_far + came[k][s - 1, d, h, at].astype(jnp.float32)
        return so_far.astype(jnp.bfloat16)

    def arrive(s, k, d, first):
        load_own(s, k, d).wait()
        give(s, k, d).wait_recv()
        if not first:
            ring(s - 1, k, d).wait_recv()

    def add(s, k, d, first):
        arrive(s, k, d, first)

        def body(h, at):
            given[k][s, d, h, at] = total(s, k, d, h, at, first)

        by_rows(k, body)
        ring(s, k, d).start()

    def update(s, k, d):
        arrive(s, k, d, False)
        for copy in load_state(k, d):
            copy.wait()

        def body(h, at):
            grad = total(s, k, d, h, at, False).astype(jnp.float32)
            one = adamw(wb[k][d, h, at].astype(jnp.float32), mb[k][d, h, at], vb[k][d, h, at], grad)
            wb[k][d, h, at], mb[k][d, h, at], vb[k][d, h, at] = one

        by_rows(k, body)
        gather(0, k, d).start()
        side(0, k, d).start()
        for copy in store_state(k, d):
            copy.start()

    barrier = pltpu.get_barrier_semaphore()
    for device in (*ahead, partner):
        pl.semaphore_signal(barrier, inc=1, device_id=device)
    for k, d in parts:
        load_own(0, k, d).start()
    pl.semaphore_wait(barrier, 3)
    for k, d in parts:
        give(0, k, d).start()
    for k, d in parts:
        load_own(1, k, d).start()
        give(1, k, d).start()

    def onward(s, k, d):
        load_own(s + 2, k, d).start()
        give(s + 2, k, d).start()

    last = chips - 1
    for k, d in parts:
        add(0, k, d, True)
        onward(0, k, d)
    for k, d in parts:
        for copy in load_state(k, d):
            copy.start()

    @pl.loop(1, last - 1)
    def _(s):
        for k, d in parts:
            add(s, k, d, False)
            onward(s, k, d)

    for k, d in parts:
        add(last - 1, k, d, False)
    for k, d in parts:
        update(last, k, d)

    @pl.loop(1, last)
    def _(t):
        for k, d in parts:
            gather_recv(t - 1, k, d).wait_recv()
            gather(t, k, d).start()
            side(t, k, d).start()

    for k, d in parts:
        gather_recv(last - 1, k, d).wait_recv()
        side(last, k, d).start()

    for k, d in parts:
        for copy in store_state(k, d):
            copy.wait()
        gather(0, k, d).wait_send()
        side(0, k, d).wait_send()

    @pl.loop(0, last)
    def _(s):
        for k, d in parts:
            give(s, k, d).wait_send()
            ring(s, k, d).wait_send()
            side_recv_of(s, k, d).wait_recv()

    @pl.loop(1, last)
    def _(t):
        for k, d in parts:
            gather(t, k, d).wait_send()
            side(t, k, d).wait_send()

    for k, d in parts:
        give(last, k, d).wait_send()
        side(last, k, d).wait_send()
        side_recv_of(last, k, d).wait_recv()


def solution(mesh):
    chips = mesh.shape["dp"] // CORES

    def step(*arrays):
        terms, weights, m, v = (arrays[i : i + 3] for i in (0, 3, 6, 9))
        count = len(weights)
        shapes = [(one.shape[0] // WAYS, *one.shape[1:]) for one in m]
        any_of = pl.BlockSpec(memory_space=pl.ANY)
        dma = pltpu.SemaphoreType.DMA
        out = pl.pallas_call(
            functools.partial(kernel, chips, count),
            out_shape=[jax.ShapeDtypeStruct(one.shape, one.dtype) for one in (*weights, *m, *v)],
            in_specs=[any_of] * len(arrays),
            out_specs=[any_of] * (3 * count),
            scratch_shapes=[
                *(pltpu.VMEM((chips, WAYS, *one), jnp.bfloat16) for one in shapes),
                *(pltpu.VMEM((chips - 1, WAYS, *one), jnp.bfloat16) for one in shapes),
                *(pltpu.VMEM((2, WAYS, *one), jnp.bfloat16) for one in shapes),
                *(pltpu.VMEM((WAYS, *one), jnp.bfloat16) for one in shapes),
                *(pltpu.VMEM((WAYS, *one), jnp.float32) for one in shapes),
                *(pltpu.VMEM((WAYS, *one), jnp.float32) for one in shapes),
                dma((2, count, WAYS)),
                dma((chips, count, WAYS)),
                dma((chips, count, WAYS)),
                dma((chips - 1, count, WAYS)),
                dma((chips - 1, count, WAYS)),
                dma((3, count, WAYS)),
                dma((3, count, WAYS)),
                dma((chips - 1, count, WAYS)),
                dma((chips - 1, count, WAYS)),
                dma((chips, count, WAYS)),
                dma((chips, count, WAYS)),
            ],
            compiler_params=pltpu.CompilerParams(collective_id=0, has_side_effects=True, vmem_limit_bytes=60 * 1024 * 1024),
        )(*terms, *weights, *m, *v)
        return tuple(out)

    all_of, cut = P(None, None, None), P(None, "dp", None)
    return jax.shard_map(
        step,
        mesh=mesh,
        in_specs=(P(("rep", "dp"), None, None, None),) * 3 + (all_of,) * 3 + (cut,) * 6,
        out_specs=(P("rep", None, None),) * 3 + (P("rep", "dp", None),) * 6,
        check_vma=False,
    )
```

```python
import functools

import jax
import jax.numpy as jnp
from jax import lax
from jax.experimental import pallas as pl
from jax.experimental.pallas import tpu as pltpu
from jax.sharding import PartitionSpec as P

CORES = 2
ROWS = 16
WAYS = 2


def adamw(w, m, v, g):
    m = 0.9 * m + 0.1 * g
    v = 0.95 * v + 0.05 * g * g
    step = m * lax.rsqrt(v + 1e-8) + 0.1 * w
    return (w - 0.02 * step).astype(jnp.bfloat16), m, v


def kernel(chips, count, *refs):
    def take(number):
        nonlocal refs
        head, refs = refs[:number], refs[number:]
        return head

    g, w, m, v = (take(count) for _ in range(4))
    w_out, m_out, v_out = (take(count) for _ in range(3))
    own, wb = (take(count) for _ in range(2))
    own_sem, give_send, give_recv, ring_send, ring_recv, in_sem, ag_send, ag_recv, side_send, side_recv, free, clear = refs

    me = lax.axis_index("dp")
    z, c = me // CORES, me % CORES
    other = 1 - c

    def chip(i):
        return (i + 2 * chips) % chips

    partner = {"dp": z * CORES + other}
    ahead = [{"dp": chip(z + 1) * CORES + c}, {"dp": chip(z - 1) * CORES + c}]
    behind = ahead[::-1]
    parts = [(k, d) for k in range(count) for d in range(WAYS)]
    half = [one.shape[0] // WAYS for one in m]
    rows = [one.shape[1] for one in m]
    last = chips - 1

    def block(k, d, chip_of, core):
        start = pl.multiple_of((chip_of * CORES + core) * rows[k], rows[k])
        return pl.ds(d * half[k], half[k]), pl.ds(start, rows[k])

    def turn(d, s):
        return chip(z - 1 - s) if d == 0 else chip(z + 1 + s)

    def load_own(s, k, d):
        layers, where = block(k, d, turn(d, s), c)
        return pltpu.make_async_copy(g[k].at[0, layers, where], own[k].at[s % 2, d], own_sem.at[s % 2, k, d])

    def give(s, k, d):
        layers, where = block(k, d, turn(d, s), other)
        return pltpu.make_async_remote_copy(
            g[k].at[0, layers, where], w_out[k].at[layers, where], give_send.at[s, k, d], give_recv.at[s, k, d], device_id=partner
        )

    def ring(s, k, d):
        layers, where = block(k, d, turn(d, s), c)
        _, there = block(k, d, turn(d, s), other)
        return pltpu.make_async_remote_copy(
            w_out[k].at[layers, where], w_out[k].at[layers, there], ring_send.at[s, k, d], ring_recv.at[s, k, d], device_id=ahead[d]
        )

    def load_state(k, d):
        layers, where = block(k, d, z, c)
        return [
            pltpu.make_async_copy(w[k].at[layers, where], wb[k].at[d], in_sem.at[0, k, d]),
            pltpu.make_async_copy(m[k].at[layers], m_out[k].at[layers], in_sem.at[1, k, d]),
            pltpu.make_async_copy(v[k].at[layers], v_out[k].at[layers], in_sem.at[2, k, d]),
        ]

    def gathered(t, k, d):
        layers, where = block(k, d, chip(z - t) if d == 0 else chip(z + t), c)
        return w_out[k].at[layers, where]

    def gather(t, k, d):
        here = gathered(t, k, d)
        return pltpu.make_async_remote_copy(here, here, ag_send.at[t, k, d], ag_recv.at[t, k, d], device_id=ahead[d])

    def side(t, k, d):
        here = gathered(t, k, d)
        return pltpu.make_async_remote_copy(here, here, side_send.at[t, k, d], side_recv.at[t, k, d], device_id=partner)

    def by_rows(k, body):
        for h in range(half[k]):

            @pl.loop(0, rows[k] // ROWS)
            def _(i):
                body(h, i * ROWS)

    def at(k, d, chip_of, core, h, row):
        start = pl.multiple_of((chip_of * CORES + core) * rows[k] + row, ROWS)
        return d * half[k] + h, pl.ds(start, ROWS)

    def total(s, k, d, h, row, first):
        mine = own[k][s % 2, d, h, pl.ds(pl.multiple_of(row, ROWS), ROWS)]
        so_far = mine.astype(jnp.float32) + w_out[k][at(k, d, turn(d, s), c, h, row)].astype(jnp.float32)
        if not first:
            so_far = so_far + w_out[k][at(k, d, turn(d, s), other, h, row)].astype(jnp.float32)
        return so_far.astype(jnp.bfloat16)

    def arrive(s, k, d, first):
        load_own(s, k, d).wait()
        give(s, k, d).wait_recv()
        if not first:
            ring(s - 1, k, d).wait_recv()

    def add(s, k, d, first):
        arrive(s, k, d, first)

        def body(h, row):
            w_out[k][at(k, d, turn(d, s), c, h, row)] = total(s, k, d, h, row, first)

        by_rows(k, body)
        ring(s, k, d).start()
        if not first:
            ring(s - 1, k, d).wait_send()

    def update(k, d):
        arrive(last, k, d, False)
        for copy in load_state(k, d):
            copy.wait()

        def body(h, row):
            grad = total(last, k, d, h, row, False).astype(jnp.float32)
            here = pl.ds(pl.multiple_of(row, ROWS), ROWS)
            state = d * half[k] + h, here
            old = wb[k][d, h, here].astype(jnp.float32)
            new = adamw(old, m_out[k][state], v_out[k][state], grad)
            w_out[k][at(k, d, z, c, h, row)], m_out[k][state], v_out[k][state] = new

        by_rows(k, body)
        pl.semaphore_wait(clear.at[0, k, d], 1)
        gather(0, k, d).start()
        pl.semaphore_signal(free.at[k, d], inc=1, device_id=partner)

    def onward(s, k, d):
        load_own(s + 2, k, d).start()
        give(s + 2, k, d).start()

    barrier = pltpu.get_barrier_semaphore()
    for device in (*ahead, partner):
        pl.semaphore_signal(barrier, inc=1, device_id=device)
    for k, d in parts:
        load_own(0, k, d).start()
    pl.semaphore_wait(barrier, 3)
    for k, d in parts:
        give(0, k, d).start()
    for k, d in parts:
        load_own(1, k, d).start()
        give(1, k, d).start()

    for k, d in parts:
        add(0, k, d, True)
        onward(0, k, d)
    for k, d in parts:
        for copy in load_state(k, d):
            copy.start()

    @pl.loop(1, last - 1)
    def _(s):
        for k, d in parts:
            add(s, k, d, False)
            onward(s, k, d)

    for k, d in parts:
        add(last - 1, k, d, False)
        pl.semaphore_signal(clear.at[0, k, d], inc=1, device_id=behind[d])
    for i, (k, d) in enumerate(parts):
        update(k, d)
        if i:
            pl.semaphore_wait(free.at[*parts[i - 1]], 1)
            side(0, *parts[i - 1]).start()
    pl.semaphore_wait(free.at[*parts[-1]], 1)
    side(0, *parts[-1]).start()
    for k, d in parts:
        ring(last - 1, k, d).wait_send()
        pl.semaphore_signal(clear.at[1, k, d], inc=1, device_id=behind[d])

    @pl.loop(1, last - 1)
    def _(t):
        for k, d in parts:
            gather(t - 1, k, d).wait_recv()
            gather(t, k, d).start()
            side(t, k, d).start()

    for k, d in parts:
        gather(last - 2, k, d).wait_recv()
        pl.semaphore_wait(clear.at[1, k, d], 1)
        gather(last - 1, k, d).start()
        side(last - 1, k, d).start()
    for k, d in parts:
        gather(last - 1, k, d).wait_recv()
        side(last, k, d).start()

    @pl.loop(0, last)
    def _(s):
        for k, d in parts:
            give(s, k, d).wait_send()
            gather(s, k, d).wait_send()
            side(s, k, d).wait_send()
            side(s, k, d).wait_recv()

    for k, d in parts:
        give(last, k, d).wait_send()
        side(last, k, d).wait_send()
        side(last, k, d).wait_recv()


def settle(count, *refs):
    sources, targets, sem = refs[:count], refs[count : 2 * count], refs[-1]
    copies = [
        pltpu.make_async_copy(source.at[layer], target.at[layer], sem.at[i, layer])
        for i, (source, target) in enumerate(zip(sources, targets))
        for layer in range(source.shape[0])
    ]
    for copy in copies:
        copy.start()
    for copy in copies:
        copy.wait()


def solution(mesh):
    chips = mesh.shape["dp"] // CORES

    def step(*arrays):
        terms, weights, m, v = (arrays[i : i + 3] for i in (0, 3, 6, 9))
        count = len(weights)
        shapes = [(one.shape[0] // WAYS, *one.shape[1:]) for one in m]
        any_of, vmem = (pl.BlockSpec(memory_space=space) for space in (pl.ANY, pltpu.VMEM))
        dma = pltpu.SemaphoreType.DMA
        out = pl.pallas_call(
            functools.partial(kernel, chips, count),
            out_shape=[pltpu.VMEM(one.shape, one.dtype) for one in (*weights, *m, *v)],
            in_specs=[any_of] * len(arrays),
            out_specs=[vmem] * (3 * count),
            scratch_shapes=[
                *(pltpu.VMEM((2, WAYS, *one), jnp.bfloat16) for one in shapes),
                *(pltpu.VMEM((WAYS, *one), jnp.bfloat16) for one in shapes),
                dma((2, count, WAYS)),
                dma((chips, count, WAYS)),
                dma((chips, count, WAYS)),
                dma((chips - 1, count, WAYS)),
                dma((chips - 1, count, WAYS)),
                dma((3, count, WAYS)),
                dma((chips - 1, count, WAYS)),
                dma((chips - 1, count, WAYS)),
                dma((chips, count, WAYS)),
                dma((chips, count, WAYS)),
                pltpu.SemaphoreType.REGULAR((count, WAYS)),
                pltpu.SemaphoreType.REGULAR((2, count, WAYS)),
            ],
            compiler_params=pltpu.CompilerParams(collective_id=0, has_side_effects=True, vmem_limit_bytes=8 * 1024 * 1024),
        )(*(pltpu.with_memory_space_constraint(one, pltpu.HBM) for one in arrays))
        layers = max(one.shape[0] for one in weights)
        return pl.pallas_call(
            functools.partial(settle, len(out)),
            out_shape=[jax.ShapeDtypeStruct(one.shape, one.dtype) for one in out],
            in_specs=[vmem] * len(out),
            out_specs=[any_of] * len(out),
            scratch_shapes=[dma((len(out), layers))],
            compiler_params=pltpu.CompilerParams(vmem_limit_bytes=2 * 1024 * 1024),
        )(*(pltpu.with_memory_space_constraint(one, pltpu.VMEM) for one in out))

    all_of, cut = P(None, None, None), P(None, "dp", None)
    return jax.shard_map(
        step,
        mesh=mesh,
        in_specs=(P(("rep", "dp"), None, None, None),) * 3 + (all_of,) * 3 + (cut,) * 6,
        out_specs=(P("rep", None, None),) * 3 + (P("rep", "dp", None),) * 6,
        check_vma=False,
    )
```

```python
import functools
import types

import jax
import jax.numpy as jnp
from jax import lax
from jax.experimental import pallas as pl
from jax.experimental.pallas import tpu as pltpu
from jax.sharding import PartitionSpec as P

CORES = 2
ROWS = 16
WAYS = 2
LATE = 1
PIECES = 4


def adamw(w, m, v, g):
    m = 0.9 * m + 0.1 * g
    v = 0.95 * v + 0.05 * g * g
    step = m * lax.rsqrt(v + 1e-8) + 0.1 * w
    return (w - 0.02 * step).astype(jnp.bfloat16), m, v


def cut(rows, pieces):
    tiles = rows // ROWS
    ends = [tiles * i // pieces * ROWS for i in range(pieces + 1)]
    return [(a, b - a) for a, b in zip(ends, ends[1:]) if b > a]


def parts_of(state, pieces):
    return [(k, d, *piece) for k, one in enumerate(state) for piece in cut(one.shape[-2], pieces) for d in range(WAYS)]


def place(chips):
    me = lax.axis_index("dp")
    z, c = me // CORES, me % CORES

    def chip(i):
        return (i + 2 * chips) % chips

    ahead = [{"dp": chip(z + 1) * CORES + c}, {"dp": chip(z - 1) * CORES + c}]
    return types.SimpleNamespace(
        chips=chips,
        last=chips - 1,
        z=z,
        c=c,
        other=1 - c,
        chip=chip,
        partner={"dp": z * CORES + 1 - c},
        ahead=ahead,
        behind=ahead[::-1],
        turn=lambda d, s: chip(z - 1 - s) if d == 0 else chip(z + 1 + s),
    )


def engine(at, parts, g, w_out, m_out, v_out, own, wb, sems, held=None):
    e = types.SimpleNamespace(parts=range(len(parts)))
    half = [one.shape[0] // WAYS for one in m_out]
    block_rows = [one.shape[1] for one in m_out]

    def layers(p):
        k, d, _, _ = parts[p]
        return pl.ds(d * half[k], half[k])

    def within(p):
        return pl.ds(parts[p][2], parts[p][3])

    def rows_of(p, chip_of, core):
        k, _, start, size = parts[p]
        return pl.ds(pl.multiple_of((chip_of * CORES + core) * block_rows[k] + start, ROWS), size)

    def slot(p, chip_of, core):
        return w_out[parts[p][0]].at[layers(p), rows_of(p, chip_of, core)]

    def load_own(s, p):
        k, d, _, _ = parts[p]
        here = g[k].at[0, layers(p), rows_of(p, at.turn(d, s), at.c)]
        return pltpu.make_async_copy(here, own[k].at[s % 2, d, :, within(p)], sems.own.at[s % 2, p])

    def give(s, p):
        k, d, _, _ = parts[p]
        if held is not None:
            kept = held[k].at[s, d, :, within(p)]
            return pltpu.make_async_copy(kept, slot(p, at.turn(d, s), at.c), sems.give_recv.at[s, p])
        where = rows_of(p, at.turn(d, s), at.other)
        return pltpu.make_async_remote_copy(
            g[k].at[0, layers(p), where],
            w_out[k].at[layers(p), where],
            sems.give_send.at[s, p],
            sems.give_recv.at[s, p],
            device_id=at.partner,
        )

    def ring(s, p):
        d = parts[p][1]
        return pltpu.make_async_remote_copy(
            slot(p, at.turn(d, s), at.c),
            slot(p, at.turn(d, s), at.other),
            sems.ring_send.at[s, p],
            sems.ring_recv.at[s, p],
            device_id=at.ahead[d],
        )

    def travelling(t, p):
        return slot(p, at.chip(at.z - t) if parts[p][1] == 0 else at.chip(at.z + t), at.c)

    def gather(t, p):
        here = travelling(t, p)
        return pltpu.make_async_remote_copy(
            here, here, sems.ag_send.at[t, p], sems.ag_recv.at[t, p], device_id=at.ahead[parts[p][1]]
        )

    def side(t, p):
        here = travelling(t, p)
        return pltpu.make_async_remote_copy(here, here, sems.side_send.at[t, p], sems.side_recv.at[t, p], device_id=at.partner)

    def by_rows(p, body):
        for h in range(half[parts[p][0]]):

            @pl.loop(0, parts[p][3] // ROWS)
            def _(i):
                body(h, i * ROWS)

    def tile(p, chip_of, core, h, row):
        k, d, start, _ = parts[p]
        first = pl.multiple_of((chip_of * CORES + core) * block_rows[k] + start + row, ROWS)
        return d * half[k] + h, pl.ds(first, ROWS)

    def total(s, p, h, row, first):
        k, d, start, _ = parts[p]
        mine = own[k][s % 2, d, h, pl.ds(pl.multiple_of(start + row, ROWS), ROWS)]
        so_far = mine.astype(jnp.float32) + w_out[k][tile(p, at.turn(d, s), at.c, h, row)].astype(jnp.float32)
        if not first:
            so_far = so_far + w_out[k][tile(p, at.turn(d, s), at.other, h, row)].astype(jnp.float32)
        return so_far.astype(jnp.bfloat16)

    def fetch(s, p):
        load_own(s, p).start()
        give(s, p).start()

    def arrive(s, p, first):
        load_own(s, p).wait()
        if held is not None:
            give(s, p).wait()
        else:
            give(s, p).wait_recv()
        if not first:
            ring(s - 1, p).wait_recv()

    def add(s, p, first=False):
        arrive(s, p, first)

        def body(h, row):
            k, d, _, _ = parts[p]
            w_out[k][tile(p, at.turn(d, s), at.c, h, row)] = total(s, p, h, row, first)

        by_rows(p, body)
        ring(s, p).start()
        if not first:
            ring(s - 1, p).wait_send()

    def load_state(p, w, m, v):
        k, d, _, _ = parts[p]
        return [
            pltpu.make_async_copy(w[k].at[layers(p), rows_of(p, at.z, at.c)], wb[k].at[d, :, within(p)], sems.state.at[0, p]),
            pltpu.make_async_copy(m[k].at[layers(p), within(p)], m_out[k].at[layers(p), within(p)], sems.state.at[1, p]),
            pltpu.make_async_copy(v[k].at[layers(p), within(p)], v_out[k].at[layers(p), within(p)], sems.state.at[2, p]),
        ]

    def update(p, w, m, v):
        arrive(at.last, p, False)
        for copy in load_state(p, w, m, v):
            copy.wait()

        def body(h, row):
            k, d, start, _ = parts[p]
            grad = total(at.last, p, h, row, False).astype(jnp.float32)
            here = pl.ds(pl.multiple_of(start + row, ROWS), ROWS)
            state = d * half[k] + h, here
            old = wb[k][d, h, here].astype(jnp.float32)
            new = adamw(old, m_out[k][state], v_out[k][state], grad)
            w_out[k][tile(p, at.z, at.c, h, row)], m_out[k][state], v_out[k][state] = new

        by_rows(p, body)

    def reduce_middle(first_step):
        @pl.loop(first_step, at.last - 1)
        def _(s):
            for p in e.parts:
                add(s, p)
                fetch(s + 2, p)

    def may_land(which, p):
        pl.semaphore_signal(sems.clear.at[which, p], inc=1, device_id=at.behind[parts[p][1]])

    def gather_after(which, t, p):
        pl.semaphore_wait(sems.clear.at[which, p], 1)
        gather(t, p).start()

    def may_side(p):
        pl.semaphore_signal(sems.free.at[p], inc=1, device_id=at.partner)

    def first_side(p):
        pl.semaphore_wait(sems.free.at[p], 1)
        side(0, p).start()

    def onward(t, p, which=None):
        gather(t - 1, p).wait_recv()
        if which is None:
            gather(t, p).start()
        else:
            gather_after(which, t, p)
        side(t, p).start()

    def end_gather():
        @pl.loop(0, at.last)
        def _(t):
            for p in e.parts:
                gather(t, p).wait_send()
                side(t, p).wait_send()
                side(t, p).wait_recv()

        for p in e.parts:
            side(at.last, p).wait_send()
            side(at.last, p).wait_recv()

    def end_give():
        @pl.loop(0, at.chips)
        def _(s):
            for p in e.parts:
                give(s, p).wait_send()

    for one in (
        fetch, add, load_state, update, reduce_middle, may_land, gather_after, may_side, first_side, onward, end_gather, end_give,
        ring, gather, side, slot, layers, within,
    ):
        setattr(e, one.__name__, one)
    return e


RING = ("own", "give_send", "give_recv", "ring_send", "ring_recv", "state")
GATHER = ("ag_send", "ag_recv", "side_send", "side_recv", "free", "clear")


def semaphores(chips, count, names):
    dma, plain = pltpu.SemaphoreType.DMA, pltpu.SemaphoreType.REGULAR
    full, less = (dma((chips, count)), dma((chips - 1, count)))
    shape = dict(
        own=dma((2, count)), give_send=full, give_recv=full, ring_send=less, ring_recv=less, state=dma((3, count)),
        ag_send=less, ag_recv=less, side_send=full, side_recv=full, free=plain((count,)), clear=plain((2, count)),
    )
    return [shape[name] for name in names]


def taker(refs):
    refs = list(refs)

    def take(number):
        head = refs[:number]
        del refs[:number]
        return head

    return take


def first_kernel(chips, early, parts, late_parts, *refs):
    take = taker(refs)
    late = LATE
    g, late_g, w, late_w = take(early), take(late), take(early), take(late)
    m, late_m, v, late_v = take(early), take(late), take(early), take(late)
    w_out, m_out, v_out = (take(early) for _ in range(3))
    held, new_w, new_m, new_v = (take(late) for _ in range(4))
    own, wb = take(early), take(early)
    late_own, late_wb, work, work_m, work_v = (take(late) for _ in range(5))
    sems = types.SimpleNamespace(**dict(zip(RING + GATHER, take(len(RING + GATHER)))))
    late_sems = types.SimpleNamespace(**dict(zip(RING, take(len(RING)))))
    hold_send, hold_recv, store = take(3)
    at = place(chips)
    last = at.last
    a = engine(at, parts, g, w_out, m_out, v_out, own, wb, sems)
    b = engine(at, late_parts, late_g, work, work_m, work_v, late_own, late_wb, late_sems, held)

    def hold(s, k, d):
        half, rows = held[k].shape[2:4]
        where = pl.ds(pl.multiple_of((at.turn(d, s) * CORES + at.other) * rows, rows), rows)
        return pltpu.make_async_remote_copy(
            late_g[k].at[0, pl.ds(d * half, half), where],
            held[k].at[s, d],
            hold_send.at[s, k, d],
            hold_recv.at[s, k, d],
            device_id=at.partner,
        )

    pairs = [(k, d) for k in range(late) for d in range(WAYS)]

    def store_new(p):
        k, d, _, _ = late_parts[p]
        rows = b.within(p)
        return [
            pltpu.make_async_copy(b.slot(p, at.z, at.c), new_w[k].at[d, :, rows], store.at[0, p]),
            pltpu.make_async_copy(work_m[k].at[b.layers(p), rows], new_m[k].at[b.layers(p), rows], store.at[1, p]),
            pltpu.make_async_copy(work_v[k].at[b.layers(p), rows], new_v[k].at[b.layers(p), rows], store.at[2, p]),
        ]

    barrier = pltpu.get_barrier_semaphore()
    for device in (*at.ahead, at.partner):
        pl.semaphore_signal(barrier, inc=1, device_id=device)
    pl.semaphore_wait(barrier, 3)
    for s in range(2):
        for p in a.parts:
            a.fetch(s, p)
    for p in a.parts:
        a.add(0, p, True)
        a.fetch(2, p)
    for p in a.parts:
        for copy in a.load_state(p, w, m, v):
            copy.start()
    a.reduce_middle(1)
    for p in a.parts:
        a.add(last - 1, p)
        a.may_land(0, p)
    for p in a.parts:
        a.update(p, w, m, v)
        a.gather_after(0, 0, p)
        a.may_side(p)
        if p:
            a.first_side(p - 1)
    a.first_side(len(parts) - 1)
    for p in a.parts:
        a.ring(last - 1, p).wait_send()
        a.may_land(1, p)

    @pl.loop(1, last - 1)
    def _(t):
        for p in a.parts:
            a.onward(t, p)
        for k, d in pairs:
            hold(t - 1, k, d).start()

    for s in range(last - 2, chips):
        for k, d in pairs:
            hold(s, k, d).start()
    for p in a.parts:
        a.onward(last - 1, p, 1)

    @pl.when(at.c == 1)
    def _():
        for s in range(2):
            for k, d in pairs:
                hold(s, k, d).wait_recv()
            for p in b.parts:
                b.fetch(s, p)
        for p in b.parts:
            b.add(0, p, True)
        for k, d in pairs:
            hold(2, k, d).wait_recv()
        for p in b.parts:
            b.fetch(2, p)

    for p in a.parts:
        a.gather(last - 1, p).wait_recv()
        a.side(last, p).start()

    @pl.loop(3, chips)
    def _(s):
        for k, d in pairs:
            hold(s, k, d).wait_recv()

    @pl.when(at.c == 1)
    def _():
        for p in b.parts:
            for copy in b.load_state(p, late_w, late_m, late_v):
                copy.start()
        b.reduce_middle(1)
        for p in b.parts:
            b.add(last - 1, p)
        for p in b.parts:
            b.update(p, late_w, late_m, late_v)
            for copy in store_new(p):
                copy.start()
        for p in b.parts:
            b.ring(last - 1, p).wait_send()
            for copy in store_new(p):
                copy.wait()

    @pl.when(at.c == 0)
    def _():
        for s in range(3):
            for k, d in pairs:
                hold(s, k, d).wait_recv()

    a.end_give()
    a.end_gather()

    @pl.loop(0, chips)
    def _(s):
        for k, d in pairs:
            hold(s, k, d).wait_send()


def second_kernel(chips, parts, *refs):
    take = taker(refs)
    count = LATE
    g, w, m, v, held, new_w, new_m, new_v = (take(count) for _ in range(8))
    take(1)
    w_out, m_out, v_out = (take(count) for _ in range(3))
    own, wb = take(count), take(count)
    sems = types.SimpleNamespace(**dict(zip(RING + GATHER, take(len(RING + GATHER)))))
    at = place(chips)
    last = at.last
    a = engine(at, parts, g, w_out, m_out, v_out, own, wb, sems, held)

    def bring(p):
        k, d, _, _ = parts[p]
        rows = a.within(p)
        return [
            pltpu.make_async_copy(new_w[k].at[d, :, rows], a.slot(p, at.z, at.c), sems.state.at[0, p]),
            pltpu.make_async_copy(new_m[k].at[a.layers(p), rows], m_out[k].at[a.layers(p), rows], sems.state.at[1, p]),
            pltpu.make_async_copy(new_v[k].at[a.layers(p), rows], v_out[k].at[a.layers(p), rows], sems.state.at[2, p]),
        ]

    barrier = pltpu.get_barrier_semaphore()
    for device in at.ahead:
        pl.semaphore_signal(barrier, inc=1, device_id=device)

    @pl.when(at.c == 0)
    def _():
        for s in range(2):
            for p in a.parts:
                a.fetch(s, p)
        pl.semaphore_wait(barrier, 2)
        pl.semaphore_signal(barrier, inc=1, device_id=at.partner)
        for p in a.parts:
            a.add(0, p, True)
            a.fetch(2, p)
        for p in a.parts:
            for copy in a.load_state(p, w, m, v):
                copy.start()
        a.reduce_middle(1)
        for p in a.parts:
            a.add(last - 1, p)
            a.may_land(0, p)
        for p in a.parts:
            a.update(p, w, m, v)
            a.gather_after(0, 0, p)
        for p in a.parts:
            a.ring(last - 1, p).wait_send()
            a.may_land(1, p)
        pl.semaphore_wait(barrier, 1)

    @pl.when(at.c == 1)
    def _():
        for p in a.parts:
            for copy in bring(p):
                copy.start()
        pl.semaphore_wait(barrier, 3)
        pl.semaphore_signal(barrier, inc=1, device_id=at.partner)
        for p in a.parts:
            for which in range(2):
                a.may_land(which, p)
        for p in a.parts:
            for copy in bring(p):
                copy.wait()
            a.gather_after(0, 0, p)

    for p in a.parts:
        a.may_side(p)
    for p in a.parts:
        a.first_side(p)

    @pl.loop(1, last - 1)
    def _(t):
        for p in a.parts:
            a.onward(t, p)

    for p in a.parts:
        a.onward(last - 1, p, 1)
    for p in a.parts:
        a.gather(last - 1, p).wait_recv()
        a.side(last, p).start()
    a.end_gather()


def settle(count, *refs):
    sources, targets, sem = refs[:count], refs[count : 2 * count], refs[-1]
    copies = [
        pltpu.make_async_copy(source.at[layer], target.at[layer], sem.at[i, layer])
        for i, (source, target) in enumerate(zip(sources, targets))
        for layer in range(source.shape[0])
    ]
    for copy in copies:
        copy.start()
    refs[2 * count][...] = jnp.zeros_like(refs[2 * count])
    for copy in copies:
        copy.wait()


def solution(mesh):
    chips = mesh.shape["dp"] // CORES
    any_of, vmem = (pl.BlockSpec(memory_space=space) for space in (pl.ANY, pltpu.VMEM))
    dma = pltpu.SemaphoreType.DMA
    mib = 1024 * 1024

    def in_hbm(arrays):
        return [pltpu.with_memory_space_constraint(one, pltpu.HBM) for one in arrays]

    def out(arrays):
        layers = max(one.shape[0] for one in arrays)
        shapes = [jax.ShapeDtypeStruct(one.shape, one.dtype) for one in arrays]
        *whole, token = pl.pallas_call(
            functools.partial(settle, len(arrays)),
            out_shape=[*shapes, jax.ShapeDtypeStruct((8, 128), jnp.float32)],
            in_specs=[vmem] * len(arrays),
            out_specs=[any_of] * len(arrays) + [vmem],
            scratch_shapes=[dma((len(arrays), layers))],
            compiler_params=pltpu.CompilerParams(vmem_limit_bytes=2 * mib),
        )(*(pltpu.with_memory_space_constraint(one, pltpu.VMEM) for one in arrays))
        return whole, token

    def step(*arrays):
        terms, weights, m, v = (arrays[i : i + 3] for i in (0, 3, 6, 9))
        early = len(weights) - LATE
        shapes = [(one.shape[0] // WAYS, *one.shape[1:]) for one in m]
        parts, late_parts = parts_of(m[:early], 1), parts_of(m[early:], PIECES)

        def slots(some, number, dtype=jnp.bfloat16):
            return [pltpu.VMEM((*number, *one), dtype) for one in some]

        late_shapes = shapes[early:]
        results = pl.pallas_call(
            functools.partial(first_kernel, chips, early, parts, late_parts),
            out_shape=[
                *(pltpu.VMEM(one.shape, one.dtype) for one in (*weights[:early], *m[:early], *v[:early])),
                *(pltpu.HBM((chips, WAYS, *one), jnp.bfloat16) for one in late_shapes),
                *(pltpu.HBM((WAYS, *one), jnp.bfloat16) for one in late_shapes),
                *(pltpu.HBM(one.shape, one.dtype) for one in (*m[early:], *v[early:])),
            ],
            in_specs=[any_of] * len(arrays),
            out_specs=[vmem] * (3 * early) + [any_of] * (4 * LATE),
            scratch_shapes=[
                *slots(shapes[:early], (2, WAYS)),
                *slots(shapes[:early], (WAYS,)),
                *slots(late_shapes, (2, WAYS)),
                *slots(late_shapes, (WAYS,)),
                *(pltpu.VMEM(one.shape, one.dtype) for one in (*weights[early:], *m[early:], *v[early:])),
                *semaphores(chips, len(parts), RING + GATHER),
                *semaphores(chips, len(late_parts), RING),
                dma((chips, LATE, WAYS)),
                dma((chips, LATE, WAYS)),
                dma((3, len(late_parts))),
            ],
            compiler_params=pltpu.CompilerParams(collective_id=0, has_side_effects=True, vmem_limit_bytes=24 * mib),
        )(*in_hbm(arrays))
        (w1, m1, v1), rest = (results[i : i + early] for i in (0, early, 2 * early)), results[3 * early :]
        done, token = out([*w1, *m1, *v1])
        late = [one for kind in (terms, weights, m, v) for one in kind[early:]]
        results = pl.pallas_call(
            functools.partial(second_kernel, chips, late_parts),
            out_shape=[pltpu.VMEM(one.shape, one.dtype) for one in (*weights[early:], *m[early:], *v[early:])],
            in_specs=[any_of] * (len(late) + len(rest) + 1),
            out_specs=[vmem] * (3 * LATE),
            scratch_shapes=[
                *slots(late_shapes, (2, WAYS)),
                *slots(late_shapes, (WAYS,)),
                *semaphores(chips, len(late_parts), RING + GATHER),
            ],
            compiler_params=pltpu.CompilerParams(collective_id=1, has_side_effects=True, vmem_limit_bytes=8 * mib),
        )(*in_hbm([*late, *rest, token]))
        then, _ = out(results)
        return tuple(
            one
            for i in range(3)
            for one in (*done[i * early : (i + 1) * early], *then[i * LATE : (i + 1) * LATE])
        )

    all_of, sharded = P(None, None, None), P(None, "dp", None)
    return jax.shard_map(
        step,
        mesh=mesh,
        in_specs=(P(("rep", "dp"), None, None, None),) * 3 + (all_of,) * 3 + (sharded,) * 6,
        out_specs=(P("rep", None, None),) * 3 + (P("rep", "dp", None),) * 6,
        check_vma=False,
    )
```

```python
import functools
import types

import jax
import jax.numpy as jnp
from jax import lax
from jax.experimental import pallas as pl
from jax.experimental.pallas import tpu as pltpu
from jax.sharding import PartitionSpec as P

CORES = 2
ROWS = 16
WAYS = 2
LATE = 1
PIECES = 4


def adamw(w, m, v, g):
    m = 0.9 * m + 0.1 * g
    v = 0.95 * v + 0.05 * g * g
    step = m * lax.rsqrt(v + 1e-8) + 0.1 * w
    return (w - 0.02 * step).astype(jnp.bfloat16), m, v


def cut(rows, pieces):
    tiles = rows // ROWS
    ends = [tiles * i // pieces * ROWS for i in range(pieces + 1)]
    return [(a, b - a) for a, b in zip(ends, ends[1:]) if b > a]


def parts_of(state, pieces):
    return [(k, d, *piece) for k, one in enumerate(state) for piece in cut(one.shape[-2], pieces) for d in range(WAYS)]


def place(chips):
    me = lax.axis_index("dp")
    z, c = me // CORES, me % CORES

    def chip(i):
        return (i + 2 * chips) % chips

    ahead = [{"dp": chip(z + 1) * CORES + c}, {"dp": chip(z - 1) * CORES + c}]
    return types.SimpleNamespace(
        chips=chips,
        last=chips - 1,
        z=z,
        c=c,
        other=1 - c,
        chip=chip,
        partner={"dp": z * CORES + 1 - c},
        ahead=ahead,
        behind=ahead[::-1],
        turn=lambda d, s: chip(z - 1 - s) if d == 0 else chip(z + 1 + s),
    )


def engine(at, parts, g, w_out, m_out, v_out, own, wb, sems, held=None):
    e = types.SimpleNamespace(parts=range(len(parts)))
    half = [one.shape[0] // WAYS for one in m_out]
    block_rows = [one.shape[1] for one in m_out]

    def layers(p):
        k, d, _, _ = parts[p]
        return pl.ds(d * half[k], half[k])

    def within(p):
        return pl.ds(parts[p][2], parts[p][3])

    def rows_of(p, chip_of, core):
        k, _, start, size = parts[p]
        return pl.ds(pl.multiple_of((chip_of * CORES + core) * block_rows[k] + start, ROWS), size)

    def slot(p, chip_of, core):
        return w_out[parts[p][0]].at[layers(p), rows_of(p, chip_of, core)]

    ways = range(WAYS)
    opens = [all(parts[q][0] != part[0] for q in range(p)) for p, part in enumerate(parts)]
    closes = [all(parts[q][0] != part[0] for q in range(p + 1, len(parts))) for p, part in enumerate(parts)]

    def all_of(k, d, chip_of, core):
        start = pl.multiple_of((chip_of * CORES + core) * block_rows[k], block_rows[k])
        return pl.ds(d * half[k], half[k]), pl.ds(start, block_rows[k])

    def blocks(k, number):
        return w_out[k].at[:, pl.ds(0, number * block_rows[k])]

    def wait_all(ref, sem):
        pltpu.make_async_copy(ref, ref, sem).wait()

    def load_own(s, k):
        for d in ways:
            here = (0, *all_of(k, d, at.turn(d, s), at.c))
            pltpu.make_async_copy(g[k].at[here], own[k].at[s % 2, d], sems.own.at[s % 2, k]).start()

    def give(s, p):
        k, d, _, _ = parts[p]
        where = rows_of(p, at.turn(d, s), at.other)
        return pltpu.make_async_remote_copy(
            g[k].at[0, layers(p), where],
            w_out[k].at[layers(p), where],
            sems.first_send.at[p],
            sems.first_recv.at[p],
            device_id=at.partner,
        )

    def give_all(s, k):
        for d in ways:
            if held is not None:
                slot_of = w_out[k].at[all_of(k, d, at.turn(d, s), at.c)]
                pltpu.make_async_copy(held[k].at[s, d], slot_of, sems.kept.at[s % 2, k]).start()
            else:
                where = all_of(k, d, at.turn(d, s), at.other)
                pltpu.make_async_remote_copy(
                    g[k].at[(0, *where)],
                    w_out[k].at[where],
                    sems.give_send.at[k],
                    sems.give_recv.at[s, k],
                    device_id=at.partner,
                ).start()

    def ring(s, p):
        d = parts[p][1]
        return pltpu.make_async_remote_copy(
            slot(p, at.turn(d, s), at.c),
            slot(p, at.turn(d, s), at.other),
            sems.ring_send.at[s % 2, p],
            sems.ring_recv.at[s, p],
            device_id=at.ahead[d],
        )

    def travelling(t, p):
        return slot(p, at.chip(at.z - t) if parts[p][1] == 0 else at.chip(at.z + t), at.c)

    def gather(t, p):
        here = travelling(t, p)
        return pltpu.make_async_remote_copy(
            here, here, sems.ag_send.at[parts[p][0]], sems.ag_recv.at[t, p], device_id=at.ahead[parts[p][1]]
        )

    def side(t, p):
        here = travelling(t, p)
        k = parts[p][0]
        return pltpu.make_async_remote_copy(here, here, sems.side_send.at[k], sems.side_recv.at[k], device_id=at.partner)

    def by_rows(p, body):
        for h in range(half[parts[p][0]]):

            @pl.loop(0, parts[p][3] // ROWS)
            def _(i):
                body(h, i * ROWS)

    def tile(p, chip_of, core, h, row):
        k, d, start, _ = parts[p]
        first = pl.multiple_of((chip_of * CORES + core) * block_rows[k] + start + row, ROWS)
        return d * half[k] + h, pl.ds(first, ROWS)

    def total(s, p, h, row, first):
        k, d, start, _ = parts[p]
        mine = own[k][s % 2, d, h, pl.ds(pl.multiple_of(start + row, ROWS), ROWS)]
        so_far = mine.astype(jnp.float32) + w_out[k][tile(p, at.turn(d, s), at.c, h, row)].astype(jnp.float32)
        if not first:
            so_far = so_far + w_out[k][tile(p, at.turn(d, s), at.other, h, row)].astype(jnp.float32)
        return so_far.astype(jnp.bfloat16)

    def fetch(s, k):
        load_own(s, k)
        give_all(s, k)

    def arrive(s, p, first):
        k = parts[p][0]
        if opens[p]:
            wait_all(own[k].at[s % 2], sems.own.at[s % 2, k])
            if held is not None:
                wait_all(blocks(k, 1), sems.kept.at[s % 2, k])
            elif not first:
                wait_all(blocks(k, 1), sems.give_recv.at[s, k])
        if first and held is None:
            give(s, p).wait_recv()
        if not first:
            ring(s - 1, p).wait_recv()

    def add(s, p, first=False, then=None):
        arrive(s, p, first)
        if then is not None:
            then()

        def body(h, row):
            k, d, _, _ = parts[p]
            w_out[k][tile(p, at.turn(d, s), at.c, h, row)] = total(s, p, h, row, first)

        by_rows(p, body)
        ring(s, p).start()
        if not first:
            ring(s - 1, p).wait_send()

    def load_state(k, w, m, v):
        for d in ways:
            here = all_of(k, d, at.z, at.c)
            pltpu.make_async_copy(w[k].at[here], wb[k].at[d], sems.state.at[0, k]).start()
        pltpu.make_async_copy(m[k], m_out[k], sems.state.at[1, k]).start()
        pltpu.make_async_copy(v[k], v_out[k], sems.state.at[2, k]).start()

    def update(p):
        arrive(at.last, p, False)
        if opens[p]:
            for i, ref in enumerate((wb, m_out, v_out)):
                wait_all(ref[parts[p][0]], sems.state.at[i, parts[p][0]])

        def body(h, row):
            k, d, start, _ = parts[p]
            grad = total(at.last, p, h, row, False).astype(jnp.float32)
            here = pl.ds(pl.multiple_of(start + row, ROWS), ROWS)
            state = d * half[k] + h, here
            old = wb[k][d, h, here].astype(jnp.float32)
            new = adamw(old, m_out[k][state], v_out[k][state], grad)
            w_out[k][tile(p, at.z, at.c, h, row)], m_out[k][state], v_out[k][state] = new

        by_rows(p, body)

    def reduce_middle(first_step):
        @pl.loop(first_step, at.last - 1)
        def _(s):
            for p in e.parts:
                add(s, p)
                if closes[p]:
                    fetch(s + 2, parts[p][0])

    def may_land(which, p):
        pl.semaphore_signal(sems.clear.at[which, p], inc=1, device_id=at.behind[parts[p][1]])

    def gather_after(which, t, p):
        pl.semaphore_wait(sems.clear.at[which, p], 1)
        gather(t, p).start()

    def may_side(p):
        pl.semaphore_signal(sems.free.at[p], inc=1, device_id=at.partner)

    def first_side(p):
        pl.semaphore_wait(sems.free.at[p], 1)
        side(0, p).start()

    def onward(t, p, which=None):
        gather(t - 1, p).wait_recv()
        if which is None:
            gather(t, p).start()
        else:
            gather_after(which, t, p)
        side(t, p).start()

    def end_gather():
        for k in range(len(w_out)):
            wait_all(blocks(k, at.last), sems.ag_send.at[k])
            wait_all(blocks(k, at.chips), sems.side_send.at[k])
            wait_all(blocks(k, at.chips), sems.side_recv.at[k])

    def end_give():
        for k in range(len(w_out)):
            wait_all(blocks(k, at.last), sems.give_send.at[k])
        for p in e.parts:
            give(0, p).wait_send()

    for one in (
        fetch, load_own, give, give_all, add, load_state, wait_all, all_of, update, reduce_middle, may_land, gather_after, may_side, first_side, onward, end_gather, end_give,
        ring, gather, side, slot, layers, within,
    ):
        setattr(e, one.__name__, one)
    return e


GIVE = ("first_send", "first_recv", "give_send", "give_recv")
KEPT = ("kept",)
RING = ("own", "ring_send", "ring_recv", "state")
GATHER = ("ag_send", "ag_recv", "side_send", "side_recv", "free", "clear")


def semaphores(chips, count, weights, names):
    dma, plain = pltpu.SemaphoreType.DMA, pltpu.SemaphoreType.REGULAR
    shape = dict(
        first_send=dma((count,)), first_recv=dma((count,)), give_send=dma((weights,)), give_recv=dma((chips, weights)),
        kept=dma((2, weights)), own=dma((2, weights)), ring_send=dma((2, count)), ring_recv=dma((chips - 1, count)),
        state=dma((3, weights)), ag_send=dma((weights,)), ag_recv=dma((chips - 1, count)), side_send=dma((weights,)),
        side_recv=dma((weights,)), free=plain((count,)), clear=plain((2, count)),
    )
    return [shape[name] for name in names]


def named(names, refs):
    return types.SimpleNamespace(**dict(zip(names, refs)))


def taker(refs):
    refs = list(refs)

    def take(number):
        head = refs[:number]
        del refs[:number]
        return head

    return take


def first_kernel(chips, early, parts, late_parts, *refs):
    take = taker(refs)
    late = LATE
    g, late_g, w, late_w = take(early), take(late), take(early), take(late)
    m, late_m, v, late_v = take(early), take(late), take(early), take(late)
    w_out, m_out, v_out = (take(early) for _ in range(3))
    held, new_w, new_m, new_v = (take(late) for _ in range(4))
    own, wb = take(early), take(early)
    late_own, late_wb, work, work_m, work_v = (take(late) for _ in range(5))
    sems, late_sems = (named(names, take(len(names))) for names in (GIVE + RING + GATHER, KEPT + RING))
    hold_send, hold_recv, store = take(3)
    at = place(chips)
    last = at.last
    a = engine(at, parts, g, w_out, m_out, v_out, own, wb, sems)
    b = engine(at, late_parts, late_g, work, work_m, work_v, late_own, late_wb, late_sems, held)

    def hold(s, k, d):
        half, rows = held[k].shape[2:4]
        where = pl.ds(pl.multiple_of((at.turn(d, s) * CORES + at.other) * rows, rows), rows)
        return pltpu.make_async_remote_copy(
            late_g[k].at[0, pl.ds(d * half, half), where],
            held[k].at[s, d],
            hold_send.at[k],
            hold_recv.at[s, k],
            device_id=at.partner,
        )

    pairs = [(k, d) for k in range(late) for d in range(WAYS)]

    def kept(s):
        for k in range(late):
            b.wait_all(held[k].at[s], hold_recv.at[s, k])

    def store_new(p):
        k, d, _, _ = late_parts[p]
        rows = b.within(p)
        return [
            pltpu.make_async_copy(b.slot(p, at.z, at.c), new_w[k].at[d, :, rows], store.at[0, k]),
            pltpu.make_async_copy(work_m[k].at[b.layers(p), rows], new_m[k].at[b.layers(p), rows], store.at[1, k]),
            pltpu.make_async_copy(work_v[k].at[b.layers(p), rows], new_v[k].at[b.layers(p), rows], store.at[2, k]),
        ]

    barrier = pltpu.get_barrier_semaphore()
    for device in (*at.ahead, at.partner):
        pl.semaphore_signal(barrier, inc=1, device_id=device)
    for s in range(2):
        for k in range(early):
            a.load_own(s, k)
    pl.semaphore_wait(barrier, 3)
    for p in a.parts:
        a.give(0, p).start()
    for k in range(early):
        a.give_all(1, k)
    for p in a.parts:
        a.add(0, p, True)
    for k in range(early):
        a.fetch(2, k)
        a.load_state(k, w, m, v)
    a.reduce_middle(1)
    for p in a.parts:
        a.add(last - 1, p)
        a.may_land(0, p)
    for p in a.parts:
        a.update(p)
        a.gather_after(0, 0, p)
        a.may_side(p)
        if p:
            a.first_side(p - 1)
    a.first_side(len(parts) - 1)
    for p in a.parts:
        a.ring(last - 1, p).wait_send()
        a.may_land(1, p)

    @pl.loop(1, last - 1)
    def _(t):
        for p in a.parts:
            a.onward(t, p)
        for k, d in pairs:
            hold(t - 1, k, d).start()

    for s in range(last - 2, chips):
        for k, d in pairs:
            hold(s, k, d).start()
    for p in a.parts:
        a.onward(last - 1, p, 1)

    @pl.when(at.c == 1)
    def _():
        for s in range(2):
            kept(s)
            for k in range(late):
                b.fetch(s, k)
        for p in b.parts:
            b.add(0, p, True)
        kept(2)
        for k in range(late):
            b.fetch(2, k)

    for p in a.parts:
        a.gather(last - 1, p).wait_recv()
        a.side(last, p).start()

    @pl.loop(3, chips)
    def _(s):
        kept(s)

    @pl.when(at.c == 1)
    def _():
        for k in range(late):
            b.load_state(k, late_w, late_m, late_v)
        b.reduce_middle(1)
        for p in b.parts:
            b.add(last - 1, p)
        for p in b.parts:
            b.update(p)
            for copy in store_new(p):
                copy.start()
        for p in b.parts:
            b.ring(last - 1, p).wait_send()
        for k in range(late):
            for i, ref in enumerate((new_w, new_m, new_v)):
                b.wait_all(ref[k], store.at[i, k])

    @pl.when(at.c == 0)
    def _():
        for s in range(3):
            kept(s)

    a.end_give()
    a.end_gather()
    for k in range(late):
        b.wait_all(held[k], hold_send.at[k])


def second_kernel(chips, parts, *refs):
    take = taker(refs)
    count = LATE
    g, w, m, v, held, new_w, new_m, new_v = (take(count) for _ in range(8))
    take(1)
    w_out, m_out, v_out = (take(count) for _ in range(3))
    own, wb = take(count), take(count)
    sems = named(KEPT + RING + GATHER, take(len(KEPT + RING + GATHER)))
    at = place(chips)
    last = at.last
    a = engine(at, parts, g, w_out, m_out, v_out, own, wb, sems, held)

    def bring(k):
        for d in range(WAYS):
            here = w_out[k].at[a.all_of(k, d, at.z, at.c)]
            pltpu.make_async_copy(new_w[k].at[d], here, sems.state.at[0, k]).start()
        pltpu.make_async_copy(new_m[k], m_out[k], sems.state.at[1, k]).start()
        pltpu.make_async_copy(new_v[k], v_out[k], sems.state.at[2, k]).start()

    barrier = pltpu.get_barrier_semaphore()
    for device in at.ahead:
        pl.semaphore_signal(barrier, inc=1, device_id=device)

    @pl.when(at.c == 0)
    def _():
        for s in range(2):
            for k in range(count):
                a.fetch(s, k)
        pl.semaphore_wait(barrier, 2)
        pl.semaphore_signal(barrier, inc=1, device_id=at.partner)
        for p in a.parts:
            a.add(0, p, True)
        for k in range(count):
            a.fetch(2, k)
            a.load_state(k, w, m, v)
        a.reduce_middle(1)
        for p in a.parts:
            a.add(last - 1, p)
            a.may_land(0, p)
        for p in a.parts:
            a.update(p)
            a.gather_after(0, 0, p)
        for p in a.parts:
            a.ring(last - 1, p).wait_send()
            a.may_land(1, p)
        pl.semaphore_wait(barrier, 1)

    @pl.when(at.c == 1)
    def _():
        for k in range(count):
            bring(k)
        pl.semaphore_wait(barrier, 3)
        pl.semaphore_signal(barrier, inc=1, device_id=at.partner)
        for p in a.parts:
            for which in range(2):
                a.may_land(which, p)
        for k in range(count):
            for i, ref in enumerate((new_w, m_out, v_out)):
                a.wait_all(ref[k], sems.state.at[i, k])
        for p in a.parts:
            a.gather_after(0, 0, p)

    for p in a.parts:
        a.may_side(p)
    for p in a.parts:
        a.first_side(p)

    @pl.loop(1, last - 1)
    def _(t):
        for p in a.parts:
            a.onward(t, p)

    for p in a.parts:
        a.onward(last - 1, p, 1)
    for p in a.parts:
        a.gather(last - 1, p).wait_recv()
        a.side(last, p).start()
    a.end_gather()


def settle(count, *refs):
    sources, targets, sem = refs[:count], refs[count : 2 * count], refs[-1]
    copies = [
        pltpu.make_async_copy(source.at[layer], target.at[layer], sem.at[i, layer])
        for i, (source, target) in enumerate(zip(sources, targets))
        for layer in range(source.shape[0])
    ]
    for copy in copies:
        copy.start()
    refs[2 * count][...] = jnp.zeros_like(refs[2 * count])
    for copy in copies:
        copy.wait()


def solution(mesh):
    chips = mesh.shape["dp"] // CORES
    any_of, vmem = (pl.BlockSpec(memory_space=space) for space in (pl.ANY, pltpu.VMEM))
    dma = pltpu.SemaphoreType.DMA
    mib = 1024 * 1024

    def in_hbm(arrays):
        return [pltpu.with_memory_space_constraint(one, pltpu.HBM) for one in arrays]

    def out(arrays):
        layers = max(one.shape[0] for one in arrays)
        shapes = [jax.ShapeDtypeStruct(one.shape, one.dtype) for one in arrays]
        *whole, token = pl.pallas_call(
            functools.partial(settle, len(arrays)),
            out_shape=[*shapes, jax.ShapeDtypeStruct((8, 128), jnp.float32)],
            in_specs=[vmem] * len(arrays),
            out_specs=[any_of] * len(arrays) + [vmem],
            scratch_shapes=[dma((len(arrays), layers))],
            compiler_params=pltpu.CompilerParams(vmem_limit_bytes=2 * mib),
        )(*(pltpu.with_memory_space_constraint(one, pltpu.VMEM) for one in arrays))
        return whole, token

    def step(*arrays):
        terms, weights, m, v = (arrays[i : i + 3] for i in (0, 3, 6, 9))
        early = len(weights) - LATE
        shapes = [(one.shape[0] // WAYS, *one.shape[1:]) for one in m]
        parts, late_parts = parts_of(m[:early], 1), parts_of(m[early:], PIECES)

        def slots(some, number, dtype=jnp.bfloat16):
            return [pltpu.VMEM((*number, *one), dtype) for one in some]

        late_shapes = shapes[early:]
        results = pl.pallas_call(
            functools.partial(first_kernel, chips, early, parts, late_parts),
            out_shape=[
                *(pltpu.VMEM(one.shape, one.dtype) for one in (*weights[:early], *m[:early], *v[:early])),
                *(pltpu.HBM((chips, WAYS, *one), jnp.bfloat16) for one in late_shapes),
                *(pltpu.HBM((WAYS, *one), jnp.bfloat16) for one in late_shapes),
                *(pltpu.HBM(one.shape, one.dtype) for one in (*m[early:], *v[early:])),
            ],
            in_specs=[any_of] * len(arrays),
            out_specs=[vmem] * (3 * early) + [any_of] * (4 * LATE),
            scratch_shapes=[
                *slots(shapes[:early], (2, WAYS)),
                *slots(shapes[:early], (WAYS,)),
                *slots(late_shapes, (2, WAYS)),
                *slots(late_shapes, (WAYS,)),
                *(pltpu.VMEM(one.shape, one.dtype) for one in (*weights[early:], *m[early:], *v[early:])),
                *semaphores(chips, len(parts), early, GIVE + RING + GATHER),
                *semaphores(chips, len(late_parts), LATE, KEPT + RING),
                dma((LATE,)),
                dma((chips, LATE)),
                dma((3, LATE)),
            ],
            compiler_params=pltpu.CompilerParams(collective_id=0, has_side_effects=True, vmem_limit_bytes=24 * mib),
        )(*in_hbm(arrays))
        (w1, m1, v1), rest = (results[i : i + early] for i in (0, early, 2 * early)), results[3 * early :]
        done, token = out([*w1, *m1, *v1])
        late = [one for kind in (terms, weights, m, v) for one in kind[early:]]
        results = pl.pallas_call(
            functools.partial(second_kernel, chips, late_parts),
            out_shape=[pltpu.VMEM(one.shape, one.dtype) for one in (*weights[early:], *m[early:], *v[early:])],
            in_specs=[any_of] * (len(late) + len(rest) + 1),
            out_specs=[vmem] * (3 * LATE),
            scratch_shapes=[
                *slots(late_shapes, (2, WAYS)),
                *slots(late_shapes, (WAYS,)),
                *semaphores(chips, len(late_parts), LATE, KEPT + RING + GATHER),
            ],
            compiler_params=pltpu.CompilerParams(collective_id=1, has_side_effects=True, vmem_limit_bytes=8 * mib),
        )(*in_hbm([*late, *rest]), token)
        then, _ = out(results)
        return tuple(
            one
            for i in range(3)
            for one in (*done[i * early : (i + 1) * early], *then[i * LATE : (i + 1) * LATE])
        )

    all_of, sharded = P(None, None, None), P(None, "dp", None)
    return jax.shard_map(
        step,
        mesh=mesh,
        in_specs=(P(("rep", "dp"), None, None, None),) * 3 + (all_of,) * 3 + (sharded,) * 6,
        out_specs=(P("rep", None, None),) * 3 + (P("rep", "dp", None),) * 6,
        check_vma=False,
    )
```

```python
import functools
import types

import jax
import jax.numpy as jnp
from jax import lax
from jax.experimental import pallas as pl
from jax.experimental.pallas import tpu as pltpu
from jax.sharding import PartitionSpec as P

CORES = 2
ROWS = 16
WAYS = 2
LATE = 1
FIRST = (1, 3)
PIECES = (1, 1, 1, 1)


def adamw(w, m, v, g):
    m = 0.9 * m + 0.1 * g
    v = 0.95 * v + 0.05 * g * g
    step = m * lax.rsqrt(v + 1e-8) + 0.1 * w
    return (w - 0.02 * step).astype(jnp.bfloat16), m, v


def cut(rows, shares):
    tiles = rows // ROWS
    ends = [tiles * sum(shares[:i]) // sum(shares) * ROWS for i in range(len(shares) + 1)]
    return [(a, b - a) for a, b in zip(ends, ends[1:]) if b > a]


def parts_of(state, shares):
    return [
        (k, d, *piece)
        for k, (one, some) in enumerate(zip(state, shares))
        for piece in cut(one.shape[-2], some)
        for d in range(WAYS)
    ]


def place(chips):
    me = lax.axis_index("dp")
    z, c = me // CORES, me % CORES

    def chip(i):
        return (i + 2 * chips) % chips

    ahead = [{"dp": chip(z + 1) * CORES + c}, {"dp": chip(z - 1) * CORES + c}]
    return types.SimpleNamespace(
        chips=chips,
        last=chips - 1,
        z=z,
        c=c,
        other=1 - c,
        chip=chip,
        partner={"dp": z * CORES + 1 - c},
        ahead=ahead,
        behind=ahead[::-1],
        turn=lambda d, s: chip(z - 1 - s) if d == 0 else chip(z + 1 + s),
    )


def engine(at, parts, g, w_out, m_out, v_out, own, wb, sems, held=None):
    e = types.SimpleNamespace(parts=range(len(parts)))
    half = [one.shape[0] // WAYS for one in m_out]
    block_rows = [one.shape[1] for one in m_out]

    def layers(p):
        k, d, _, _ = parts[p]
        return pl.ds(d * half[k], half[k])

    def within(p):
        return pl.ds(parts[p][2], parts[p][3])

    def rows_of(p, chip_of, core):
        k, _, start, size = parts[p]
        return pl.ds(pl.multiple_of((chip_of * CORES + core) * block_rows[k] + start, ROWS), size)

    def slot(p, chip_of, core):
        return w_out[parts[p][0]].at[layers(p), rows_of(p, chip_of, core)]

    ways = range(WAYS)
    opens = [all(parts[q][0] != part[0] for q in range(p)) for p, part in enumerate(parts)]
    closes = [all(parts[q][0] != part[0] for q in range(p + 1, len(parts))) for p, part in enumerate(parts)]

    def all_of(k, d, chip_of, core):
        start = pl.multiple_of((chip_of * CORES + core) * block_rows[k], block_rows[k])
        return pl.ds(d * half[k], half[k]), pl.ds(start, block_rows[k])

    def blocks(k, number):
        return w_out[k].at[:, pl.ds(0, number * block_rows[k])]

    def wait_all(ref, sem):
        pltpu.make_async_copy(ref, ref, sem).wait()

    def load_own(s, k):
        for d in ways:
            here = (0, *all_of(k, d, at.turn(d, s), at.c))
            pltpu.make_async_copy(g[k].at[here], own[k].at[s % 2, d], sems.own.at[s % 2, k]).start()

    def give(s, p):
        k, d, _, _ = parts[p]
        where = rows_of(p, at.turn(d, s), at.other)
        return pltpu.make_async_remote_copy(
            g[k].at[0, layers(p), where],
            w_out[k].at[layers(p), where],
            sems.first_send.at[p],
            sems.first_recv.at[p],
            device_id=at.partner,
        )

    def give_all(s, k):
        for d in ways:
            if held is not None:
                slot_of = w_out[k].at[all_of(k, d, at.turn(d, s), at.c)]
                pltpu.make_async_copy(held[k].at[s, d], slot_of, sems.kept.at[s % 2, k]).start()
            else:
                where = all_of(k, d, at.turn(d, s), at.other)
                pltpu.make_async_remote_copy(
                    g[k].at[(0, *where)],
                    w_out[k].at[where],
                    sems.give_send.at[k],
                    sems.give_recv.at[s, k],
                    device_id=at.partner,
                ).start()

    def ring(s, p):
        d = parts[p][1]
        return pltpu.make_async_remote_copy(
            slot(p, at.turn(d, s), at.c),
            slot(p, at.turn(d, s), at.other),
            sems.ring_send.at[s % 2, p],
            sems.ring_recv.at[s, p],
            device_id=at.ahead[d],
        )

    def travelling(t, p):
        return slot(p, at.chip(at.z - t) if parts[p][1] == 0 else at.chip(at.z + t), at.c)

    def gather(t, p):
        here = travelling(t, p)
        return pltpu.make_async_remote_copy(
            here, here, sems.ag_send.at[parts[p][0]], sems.ring_recv.at[t, p], device_id=at.ahead[parts[p][1]]
        )

    def side(t, p):
        here = travelling(t, p)
        k = parts[p][0]
        return pltpu.make_async_remote_copy(here, here, sems.side_send.at[k], sems.side_recv.at[k], device_id=at.partner)

    def by_rows(p, body):
        for h in range(half[parts[p][0]]):

            @pl.loop(0, parts[p][3] // ROWS)
            def _(i):
                body(h, i * ROWS)

    def tile(p, chip_of, core, h, row):
        k, d, start, _ = parts[p]
        first = pl.multiple_of((chip_of * CORES + core) * block_rows[k] + start + row, ROWS)
        return d * half[k] + h, pl.ds(first, ROWS)

    def total(s, p, h, row, first):
        k, d, start, _ = parts[p]
        mine = own[k][s % 2, d, h, pl.ds(pl.multiple_of(start + row, ROWS), ROWS)]
        so_far = mine.astype(jnp.float32) + w_out[k][tile(p, at.turn(d, s), at.c, h, row)].astype(jnp.float32)
        if not first:
            so_far = so_far + w_out[k][tile(p, at.turn(d, s), at.other, h, row)].astype(jnp.float32)
        return so_far.astype(jnp.bfloat16)

    def fetch(s, k):
        load_own(s, k)
        give_all(s, k)

    def arrive(s, p, first):
        k = parts[p][0]
        if opens[p]:
            wait_all(own[k].at[s % 2], sems.own.at[s % 2, k])
            if held is not None:
                wait_all(blocks(k, 1), sems.kept.at[s % 2, k])
            elif not first:
                wait_all(blocks(k, 1), sems.give_recv.at[s, k])
        if first and held is None:
            give(s, p).wait_recv()
        if not first:
            ring(s - 1, p).wait_recv()

    def add(s, p, first=False, then=None):
        arrive(s, p, first)
        if then is not None:
            then()

        def body(h, row):
            k, d, _, _ = parts[p]
            w_out[k][tile(p, at.turn(d, s), at.c, h, row)] = total(s, p, h, row, first)

        by_rows(p, body)
        ring(s, p).start()
        if not first:
            ring(s - 1, p).wait_send()

    def load_state(k, w, m, v):
        for d in ways:
            here = all_of(k, d, at.z, at.c)
            pltpu.make_async_copy(w[k].at[here], wb[k].at[d], sems.state.at[0, k]).start()
        pltpu.make_async_copy(m[k], m_out[k], sems.state.at[1, k]).start()
        pltpu.make_async_copy(v[k], v_out[k], sems.state.at[2, k]).start()

    def update(p):
        arrive(at.last, p, False)
        if opens[p]:
            for i, ref in enumerate((wb, m_out, v_out)):
                wait_all(ref[parts[p][0]], sems.state.at[i, parts[p][0]])

        def body(h, row):
            k, d, start, _ = parts[p]
            grad = total(at.last, p, h, row, False).astype(jnp.float32)
            here = pl.ds(pl.multiple_of(start + row, ROWS), ROWS)
            state = d * half[k] + h, here
            old = wb[k][d, h, here].astype(jnp.float32)
            new = adamw(old, m_out[k][state], v_out[k][state], grad)
            w_out[k][tile(p, at.z, at.c, h, row)], m_out[k][state], v_out[k][state] = new

        by_rows(p, body)

    def reduce_middle(first_step):
        @pl.loop(first_step, at.last - 1)
        def _(s):
            for p in e.parts:
                add(s, p)
                if closes[p]:
                    fetch(s + 2, parts[p][0])

    def may_land(which, p):
        pl.semaphore_signal(sems.clear.at[which, p], inc=1, device_id=at.behind[parts[p][1]])

    def gather_after(which, t, p):
        pl.semaphore_wait(sems.clear.at[which, p], 1)
        gather(t, p).start()

    def may_side(p):
        pl.semaphore_signal(sems.free.at[p], inc=1, device_id=at.partner)

    def first_side(p):
        pl.semaphore_wait(sems.free.at[p], 1)
        side(0, p).start()

    def onward(t, p, which=None):
        gather(t - 1, p).wait_recv()
        if which is None:
            gather(t, p).start()
        else:
            gather_after(which, t, p)
        side(t, p).start()

    def end_gather():
        for k in range(len(w_out)):
            wait_all(blocks(k, at.last), sems.ag_send.at[k])
            wait_all(blocks(k, at.chips), sems.side_send.at[k])
            wait_all(blocks(k, at.chips), sems.side_recv.at[k])

    def end_give():
        for k in range(len(w_out)):
            wait_all(blocks(k, at.last), sems.give_send.at[k])
        for p in e.parts:
            give(0, p).wait_send()

    for one in (
        fetch, load_own, give, give_all, add, load_state, wait_all, all_of, update, reduce_middle, may_land, gather_after, may_side, first_side, onward, end_gather, end_give,
        ring, gather, side, slot, layers, within,
    ):
        setattr(e, one.__name__, one)
    return e


GIVE = ("first_send", "first_recv", "give_send", "give_recv")
KEPT = ("kept",)
RING = ("own", "ring_send", "ring_recv", "state")
GATHER = ("ag_send", "side_send", "side_recv", "free", "clear")


def semaphores(chips, count, weights, names):
    dma, plain = pltpu.SemaphoreType.DMA, pltpu.SemaphoreType.REGULAR
    shape = dict(
        first_send=dma((count,)), first_recv=dma((count,)), give_send=dma((weights,)), give_recv=dma((chips, weights)),
        kept=dma((2, weights)), own=dma((2, weights)), ring_send=dma((2, count)), ring_recv=dma((chips - 1, count)),
        state=dma((3, weights)), ag_send=dma((weights,)), side_send=dma((weights,)),
        side_recv=dma((weights,)), free=plain((count,)), clear=plain((2, count)),
    )
    return [shape[name] for name in names]


def named(names, refs):
    return types.SimpleNamespace(**dict(zip(names, refs)))


def taker(refs):
    refs = list(refs)

    def take(number):
        head = refs[:number]
        del refs[:number]
        return head

    return take


def first_kernel(chips, early, parts, late_parts, *refs):
    take = taker(refs)
    late = LATE
    g, late_g, w, late_w = take(early), take(late), take(early), take(late)
    m, late_m, v, late_v = take(early), take(late), take(early), take(late)
    w_out, m_out, v_out = (take(early) for _ in range(3))
    held, new_w, new_m, new_v = (take(late) for _ in range(4))
    own, wb = take(early), take(early)
    late_own, late_wb, work, work_m, work_v = (take(late) for _ in range(5))
    sems, late_sems = (named(names, take(len(names))) for names in (GIVE + RING + GATHER, KEPT + RING))
    hold_send, hold_recv, store = take(3)
    at = place(chips)
    last = at.last
    a = engine(at, parts, g, w_out, m_out, v_out, own, wb, sems)
    b = engine(at, late_parts, late_g, work, work_m, work_v, late_own, late_wb, late_sems, held)

    def hold(s, k, d):
        half, rows = held[k].shape[2:4]
        where = pl.ds(pl.multiple_of((at.turn(d, s) * CORES + at.other) * rows, rows), rows)
        return pltpu.make_async_remote_copy(
            late_g[k].at[0, pl.ds(d * half, half), where],
            held[k].at[s, d],
            hold_send.at[k],
            hold_recv.at[s, k],
            device_id=at.partner,
        )

    pairs = [(k, d) for k in range(late) for d in range(WAYS)]

    def kept(s):
        for k in range(late):
            b.wait_all(held[k].at[s], hold_recv.at[s, k])

    def store_new(p):
        k, d, _, _ = late_parts[p]
        rows = b.within(p)
        return [
            pltpu.make_async_copy(b.slot(p, at.z, at.c), new_w[k].at[d, :, rows], store.at[0, k]),
            pltpu.make_async_copy(work_m[k].at[b.layers(p), rows], new_m[k].at[b.layers(p), rows], store.at[1, k]),
            pltpu.make_async_copy(work_v[k].at[b.layers(p), rows], new_v[k].at[b.layers(p), rows], store.at[2, k]),
        ]

    barrier = pltpu.get_barrier_semaphore()
    for device in (*at.ahead, at.partner):
        pl.semaphore_signal(barrier, inc=1, device_id=device)
    for s in range(2):
        for k in range(early):
            a.load_own(s, k)
    pl.semaphore_wait(barrier, 3)
    for p in a.parts:
        a.give(0, p).start()
    for k in range(early):
        a.give_all(1, k)
    for p in a.parts:
        a.add(0, p, True)
    for k in range(early):
        a.fetch(2, k)
        a.load_state(k, w, m, v)
    a.reduce_middle(1)
    for p in a.parts:
        a.add(last - 1, p)
        a.may_land(0, p)
    for p in a.parts:
        a.update(p)
        a.gather_after(0, 0, p)
        a.may_side(p)
        if p:
            a.first_side(p - 1)
    a.first_side(len(parts) - 1)
    for p in a.parts:
        a.ring(last - 1, p).wait_send()
        a.may_land(1, p)

    @pl.loop(1, last - 1)
    def _(t):
        for p in a.parts:
            a.onward(t, p)
        for k, d in pairs:
            hold(t - 1, k, d).start()

    for s in range(last - 2, chips):
        for k, d in pairs:
            hold(s, k, d).start()
    for p in a.parts:
        a.onward(last - 1, p, 1)

    @pl.when(at.c == 1)
    def _():
        for s in range(2):
            kept(s)
            for k in range(late):
                b.fetch(s, k)
        for p in b.parts:
            b.add(0, p, True)
        kept(2)
        for k in range(late):
            b.fetch(2, k)

    for p in a.parts:
        a.gather(last - 1, p).wait_recv()
        a.side(last, p).start()

    @pl.loop(3, chips)
    def _(s):
        kept(s)

    @pl.when(at.c == 1)
    def _():
        for k in range(late):
            b.load_state(k, late_w, late_m, late_v)
        b.reduce_middle(1)
        for p in b.parts:
            b.add(last - 1, p)
        for p in b.parts:
            b.update(p)
            for copy in store_new(p):
                copy.start()
        for p in b.parts:
            b.ring(last - 1, p).wait_send()
        for k in range(late):
            for i, ref in enumerate((new_w, new_m, new_v)):
                b.wait_all(ref[k], store.at[i, k])

    @pl.when(at.c == 0)
    def _():
        for s in range(3):
            kept(s)

    a.end_give()
    a.end_gather()
    for k in range(late):
        b.wait_all(held[k], hold_send.at[k])


def second_kernel(chips, parts, *refs):
    take = taker(refs)
    count = LATE
    g, w, m, v, held, new_w, new_m, new_v = (take(count) for _ in range(8))
    take(1)
    w_out, m_out, v_out = (take(count) for _ in range(3))
    own, wb = take(count), take(count)
    sems = named(KEPT + RING + GATHER, take(len(KEPT + RING + GATHER)))
    at = place(chips)
    last = at.last
    a = engine(at, parts, g, w_out, m_out, v_out, own, wb, sems, held)

    def bring(k):
        for d in range(WAYS):
            here = w_out[k].at[a.all_of(k, d, at.z, at.c)]
            pltpu.make_async_copy(new_w[k].at[d], here, sems.state.at[0, k]).start()
        pltpu.make_async_copy(new_m[k], m_out[k], sems.state.at[1, k]).start()
        pltpu.make_async_copy(new_v[k], v_out[k], sems.state.at[2, k]).start()

    barrier = pltpu.get_barrier_semaphore()
    for device in at.ahead:
        pl.semaphore_signal(barrier, inc=1, device_id=device)

    @pl.when(at.c == 0)
    def _():
        for s in range(2):
            for k in range(count):
                a.fetch(s, k)
        pl.semaphore_wait(barrier, 2)
        pl.semaphore_signal(barrier, inc=1, device_id=at.partner)
        for p in a.parts:
            a.add(0, p, True)
        for k in range(count):
            a.fetch(2, k)
            a.load_state(k, w, m, v)
        a.reduce_middle(1)
        for p in a.parts:
            a.add(last - 1, p)
            a.may_land(0, p)
        for p in a.parts:
            a.update(p)
            a.gather_after(0, 0, p)
        for p in a.parts:
            a.ring(last - 1, p).wait_send()
            a.may_land(1, p)
        pl.semaphore_wait(barrier, 1)

    @pl.when(at.c == 1)
    def _():
        for k in range(count):
            bring(k)
        pl.semaphore_wait(barrier, 3)
        pl.semaphore_signal(barrier, inc=1, device_id=at.partner)
        for p in a.parts:
            for which in range(2):
                a.may_land(which, p)
        for k in range(count):
            for i, ref in enumerate((new_w, m_out, v_out)):
                a.wait_all(ref[k], sems.state.at[i, k])
        for p in a.parts:
            a.gather_after(0, 0, p)

    for p in a.parts:
        a.may_side(p)
    for p in a.parts:
        a.first_side(p)

    @pl.loop(1, last - 1)
    def _(t):
        for p in a.parts:
            a.onward(t, p)

    for p in a.parts:
        a.onward(last - 1, p, 1)
    for p in a.parts:
        a.gather(last - 1, p).wait_recv()
        a.side(last, p).start()
    a.end_gather()


def settle(count, *refs):
    sources, targets, sem = refs[:count], refs[count : 2 * count], refs[-1]
    copies = [
        pltpu.make_async_copy(source.at[layer], target.at[layer], sem.at[i, layer])
        for i, (source, target) in enumerate(zip(sources, targets))
        for layer in range(source.shape[0])
    ]
    for copy in copies:
        copy.start()
    refs[2 * count][...] = jnp.zeros_like(refs[2 * count])
    for copy in copies:
        copy.wait()


def solution(mesh):
    chips = mesh.shape["dp"] // CORES
    any_of, vmem = (pl.BlockSpec(memory_space=space) for space in (pl.ANY, pltpu.VMEM))
    dma = pltpu.SemaphoreType.DMA
    mib = 1024 * 1024

    def in_hbm(arrays):
        return [pltpu.with_memory_space_constraint(one, pltpu.HBM) for one in arrays]

    def out(arrays):
        layers = max(one.shape[0] for one in arrays)
        shapes = [jax.ShapeDtypeStruct(one.shape, one.dtype) for one in arrays]
        *whole, token = pl.pallas_call(
            functools.partial(settle, len(arrays)),
            out_shape=[*shapes, jax.ShapeDtypeStruct((8, 128), jnp.float32)],
            in_specs=[vmem] * len(arrays),
            out_specs=[any_of] * len(arrays) + [vmem],
            scratch_shapes=[dma((len(arrays), layers))],
            compiler_params=pltpu.CompilerParams(vmem_limit_bytes=2 * mib),
        )(*(pltpu.with_memory_space_constraint(one, pltpu.VMEM) for one in arrays))
        return whole, token

    def step(*arrays):
        terms, weights, m, v = (arrays[i : i + 3] for i in (0, 3, 6, 9))
        early = len(weights) - LATE
        shapes = [(one.shape[0] // WAYS, *one.shape[1:]) for one in m]
        parts, late_parts = parts_of(m[:early], [FIRST] + [(1,)] * (early - 1)), parts_of(m[early:], [PIECES] * LATE)

        def slots(some, number, dtype=jnp.bfloat16):
            return [pltpu.VMEM((*number, *one), dtype) for one in some]

        late_shapes = shapes[early:]
        results = pl.pallas_call(
            functools.partial(first_kernel, chips, early, parts, late_parts),
            out_shape=[
                *(pltpu.VMEM(one.shape, one.dtype) for one in (*weights[:early], *m[:early], *v[:early])),
                *(pltpu.HBM((chips, WAYS, *one), jnp.bfloat16) for one in late_shapes),
                *(pltpu.HBM((WAYS, *one), jnp.bfloat16) for one in late_shapes),
                *(pltpu.HBM(one.shape, one.dtype) for one in (*m[early:], *v[early:])),
            ],
            in_specs=[any_of] * len(arrays),
            out_specs=[vmem] * (3 * early) + [any_of] * (4 * LATE),
            scratch_shapes=[
                *slots(shapes[:early], (2, WAYS)),
                *slots(shapes[:early], (WAYS,)),
                *slots(late_shapes, (2, WAYS)),
                *slots(late_shapes, (WAYS,)),
                *(pltpu.VMEM(one.shape, one.dtype) for one in (*weights[early:], *m[early:], *v[early:])),
                *semaphores(chips, len(parts), early, GIVE + RING + GATHER),
                *semaphores(chips, len(late_parts), LATE, KEPT + RING),
                dma((LATE,)),
                dma((chips, LATE)),
                dma((3, LATE)),
            ],
            compiler_params=pltpu.CompilerParams(collective_id=0, has_side_effects=True, vmem_limit_bytes=24 * mib),
        )(*in_hbm(arrays))
        (w1, m1, v1), rest = (results[i : i + early] for i in (0, early, 2 * early)), results[3 * early :]
        done, token = out([*w1, *m1, *v1])
        late = [one for kind in (terms, weights, m, v) for one in kind[early:]]
        results = pl.pallas_call(
            functools.partial(second_kernel, chips, late_parts),
            out_shape=[pltpu.VMEM(one.shape, one.dtype) for one in (*weights[early:], *m[early:], *v[early:])],
            in_specs=[any_of] * (len(late) + len(rest) + 1),
            out_specs=[vmem] * (3 * LATE),
            scratch_shapes=[
                *slots(late_shapes, (2, WAYS)),
                *slots(late_shapes, (WAYS,)),
                *semaphores(chips, len(late_parts), LATE, KEPT + RING + GATHER),
            ],
            compiler_params=pltpu.CompilerParams(collective_id=1, has_side_effects=True, vmem_limit_bytes=8 * mib),
        )(*in_hbm([*late, *rest]), token)
        then, _ = out(results)
        return tuple(
            one
            for i in range(3)
            for one in (*done[i * early : (i + 1) * early], *then[i * LATE : (i + 1) * LATE])
        )

    all_of, sharded = P(None, None, None), P(None, "dp", None)
    return jax.shard_map(
        step,
        mesh=mesh,
        in_specs=(P(("rep", "dp"), None, None, None),) * 3 + (all_of,) * 3 + (sharded,) * 6,
        out_specs=(P("rep", None, None),) * 3 + (P("rep", "dp", None),) * 6,
        check_vma=False,
    )
```

```python
import functools
import types

import jax
import jax.numpy as jnp
from jax import lax
from jax.experimental import pallas as pl
from jax.experimental.pallas import tpu as pltpu
from jax.sharding import PartitionSpec as P

CORES = 2
ROWS = 16
WAYS = 2
LATE = 1
FIRST = (1, 3)
PIECES = (1, 1, 1, 1)


def adamw(w, m, v, g):
    m = 0.9 * m + 0.1 * g
    v = 0.95 * v + 0.05 * g * g
    step = m * lax.rsqrt(v + 1e-8) + 0.1 * w
    return (w - 0.02 * step).astype(jnp.bfloat16), m, v


def cut(rows, shares):
    tiles = rows // ROWS
    ends = [tiles * sum(shares[:i]) // sum(shares) * ROWS for i in range(len(shares) + 1)]
    return [(a, b - a) for a, b in zip(ends, ends[1:]) if b > a]


def parts_of(state, shares):
    return [
        (k, d, *piece)
        for k, (one, some) in enumerate(zip(state, shares))
        for piece in cut(one.shape[-2], some)
        for d in range(WAYS)
    ]


def place(chips):
    me = lax.axis_index("dp")
    z, c = me // CORES, me % CORES

    def chip(i):
        return (i + 2 * chips) % chips

    ahead = [{"dp": chip(z + 1) * CORES + c}, {"dp": chip(z - 1) * CORES + c}]
    return types.SimpleNamespace(
        chips=chips,
        last=chips - 1,
        z=z,
        c=c,
        other=1 - c,
        chip=chip,
        partner={"dp": z * CORES + 1 - c},
        ahead=ahead,
        behind=ahead[::-1],
        turn=lambda d, s: chip(z - 1 - s) if d == 0 else chip(z + 1 + s),
    )


def engine(at, parts, g, w_out, m_out, v_out, own, wb, sems, held=None):
    e = types.SimpleNamespace(parts=range(len(parts)))
    half = [one.shape[0] // WAYS for one in m_out]
    block_rows = [one.shape[1] for one in m_out]

    def layers(p):
        k, d, _, _ = parts[p]
        return pl.ds(d * half[k], half[k])

    def within(p):
        return pl.ds(parts[p][2], parts[p][3])

    def rows_of(p, chip_of, core):
        k, _, start, size = parts[p]
        return pl.ds(pl.multiple_of((chip_of * CORES + core) * block_rows[k] + start, ROWS), size)

    def slot(p, chip_of, core):
        return w_out[parts[p][0]].at[layers(p), rows_of(p, chip_of, core)]

    ways = range(WAYS)
    opens = [all(parts[q][0] != part[0] for q in range(p)) for p, part in enumerate(parts)]
    closes = [all(parts[q][0] != part[0] for q in range(p + 1, len(parts))) for p, part in enumerate(parts)]

    def all_of(k, d, chip_of, core):
        start = pl.multiple_of((chip_of * CORES + core) * block_rows[k], block_rows[k])
        return pl.ds(d * half[k], half[k]), pl.ds(start, block_rows[k])

    def blocks(k, number):
        return w_out[k].at[:, pl.ds(0, number * block_rows[k])]

    def wait_all(ref, sem):
        pltpu.make_async_copy(ref, ref, sem).wait()

    def load_own(s, k):
        for d in ways:
            here = (0, *all_of(k, d, at.turn(d, s), at.c))
            pltpu.make_async_copy(g[k].at[here], own[k].at[s % 2, d], sems.own.at[s % 2, k]).start()

    def give(s, p):
        k, d, _, _ = parts[p]
        where = rows_of(p, at.turn(d, s), at.other)
        return pltpu.make_async_remote_copy(
            g[k].at[0, layers(p), where],
            w_out[k].at[layers(p), where],
            sems.first_send.at[p],
            sems.first_recv.at[p],
            device_id=at.partner,
        )

    def give_all(s, k):
        for d in ways:
            if held is not None:
                slot_of = w_out[k].at[all_of(k, d, at.turn(d, s), at.c)]
                pltpu.make_async_copy(held[k].at[s, d], slot_of, sems.kept.at[s % 2, k]).start()
            else:
                where = all_of(k, d, at.turn(d, s), at.other)
                pltpu.make_async_remote_copy(
                    g[k].at[(0, *where)],
                    w_out[k].at[where],
                    sems.give_send.at[k],
                    sems.give_recv.at[s, k],
                    device_id=at.partner,
                ).start()

    def ring(s, p):
        d = parts[p][1]
        return pltpu.make_async_remote_copy(
            slot(p, at.turn(d, s), at.c),
            slot(p, at.turn(d, s), at.other),
            sems.ring_send.at[s % 2, p],
            sems.ring_recv.at[s, p],
            device_id=at.ahead[d],
        )

    def travelling(t, p):
        return slot(p, at.chip(at.z - t) if parts[p][1] == 0 else at.chip(at.z + t), at.c)

    def gather(t, p):
        here = travelling(t, p)
        return pltpu.make_async_remote_copy(
            here, here, sems.ag_send.at[parts[p][0]], sems.ring_recv.at[t, p], device_id=at.ahead[parts[p][1]]
        )

    def side(t, p):
        here = travelling(t, p)
        k = parts[p][0]
        return pltpu.make_async_remote_copy(here, here, sems.side_send.at[k], sems.side_recv.at[k], device_id=at.partner)

    def by_rows(p, body):
        for h in range(half[parts[p][0]]):

            @pl.loop(0, parts[p][3] // ROWS)
            def _(i):
                body(h, i * ROWS)

    def tile(p, chip_of, core, h, row):
        k, d, start, _ = parts[p]
        first = pl.multiple_of((chip_of * CORES + core) * block_rows[k] + start + row, ROWS)
        return d * half[k] + h, pl.ds(first, ROWS)

    def total(s, p, h, row, first):
        k, d, start, _ = parts[p]
        mine = own[k][s % 2, d, h, pl.ds(pl.multiple_of(start + row, ROWS), ROWS)]
        so_far = mine.astype(jnp.float32) + w_out[k][tile(p, at.turn(d, s), at.c, h, row)].astype(jnp.float32)
        if not first:
            so_far = so_far + w_out[k][tile(p, at.turn(d, s), at.other, h, row)].astype(jnp.float32)
        return so_far.astype(jnp.bfloat16)

    def fetch(s, k):
        load_own(s, k)
        give_all(s, k)

    def arrive(s, p, first):
        k = parts[p][0]
        if opens[p]:
            wait_all(own[k].at[s % 2], sems.own.at[s % 2, k])
            if held is not None:
                wait_all(blocks(k, 1), sems.kept.at[s % 2, k])
            elif not first:
                wait_all(blocks(k, 1), sems.give_recv.at[s, k])
        if first and held is None:
            give(s, p).wait_recv()
        if not first:
            ring(s - 1, p).wait_recv()

    def add(s, p, first=False, then=None):
        arrive(s, p, first)
        if then is not None:
            then()

        def body(h, row):
            k, d, _, _ = parts[p]
            w_out[k][tile(p, at.turn(d, s), at.c, h, row)] = total(s, p, h, row, first)

        by_rows(p, body)
        ring(s, p).start()
        if not first:
            ring(s - 1, p).wait_send()

    def load_state(k, w, m, v):
        for d in ways:
            here = all_of(k, d, at.z, at.c)
            pltpu.make_async_copy(w[k].at[here], wb[k].at[d], sems.state.at[0, k]).start()
        pltpu.make_async_copy(m[k], m_out[k], sems.state.at[1, k]).start()
        pltpu.make_async_copy(v[k], v_out[k], sems.state.at[2, k]).start()

    def update(p):
        arrive(at.last, p, False)
        if opens[p]:
            for i, ref in enumerate((wb, m_out, v_out)):
                wait_all(ref[parts[p][0]], sems.state.at[i, parts[p][0]])

        def body(h, row):
            k, d, start, _ = parts[p]
            grad = total(at.last, p, h, row, False).astype(jnp.float32)
            here = pl.ds(pl.multiple_of(start + row, ROWS), ROWS)
            state = d * half[k] + h, here
            old = wb[k][d, h, here].astype(jnp.float32)
            new = adamw(old, m_out[k][state], v_out[k][state], grad)
            w_out[k][tile(p, at.z, at.c, h, row)], m_out[k][state], v_out[k][state] = new

        by_rows(p, body)

    def reduce_middle(first_step):
        @pl.loop(first_step, at.last - 1)
        def _(s):
            for p in e.parts:
                add(s, p)
                if closes[p]:
                    fetch(s + 2, parts[p][0])

    def may_land(which, p):
        pl.semaphore_signal(sems.clear.at[which, p], inc=1, device_id=at.behind[parts[p][1]])

    def gather_after(which, t, p):
        pl.semaphore_wait(sems.clear.at[which, p], 1)
        gather(t, p).start()

    def may_side(p):
        pl.semaphore_signal(sems.free.at[p], inc=1, device_id=at.partner)

    def first_side(p):
        pl.semaphore_wait(sems.free.at[p], 1)
        side(0, p).start()

    def onward(t, p, which=None):
        gather(t - 1, p).wait_recv()
        if which is None:
            gather(t, p).start()
        else:
            gather_after(which, t, p)
        side(t, p).start()

    def end_gather():
        for k in range(len(w_out)):
            wait_all(blocks(k, at.last), sems.ag_send.at[k])
            wait_all(blocks(k, at.chips), sems.side_send.at[k])
            wait_all(blocks(k, at.chips), sems.side_recv.at[k])

    def end_give():
        for k in range(len(w_out)):
            wait_all(blocks(k, at.last), sems.give_send.at[k])
        for p in e.parts:
            give(0, p).wait_send()

    for one in (
        fetch, load_own, give, give_all, add, load_state, wait_all, all_of, update, reduce_middle, may_land, gather_after, may_side, first_side, onward, end_gather, end_give,
        ring, gather, side, slot, layers, within,
    ):
        setattr(e, one.__name__, one)
    return e


GIVE = ("first_send", "first_recv", "give_send", "give_recv")
KEPT = ("kept",)
RING = ("own", "ring_send", "ring_recv", "state")
GATHER = ("ag_send", "side_send", "side_recv", "free", "clear")


def semaphores(chips, count, weights, names):
    dma, plain = pltpu.SemaphoreType.DMA, pltpu.SemaphoreType.REGULAR
    shape = dict(
        first_send=dma((count,)), first_recv=dma((count,)), give_send=dma((weights,)), give_recv=dma((chips, weights)),
        kept=dma((2, weights)), own=dma((2, weights)), ring_send=dma((2, count)), ring_recv=dma((chips - 1, count)),
        state=dma((3, weights)), ag_send=dma((weights,)), side_send=dma((weights,)),
        side_recv=dma((weights,)), free=plain((count,)), clear=plain((2, count)),
    )
    return [shape[name] for name in names]


def named(names, refs):
    return types.SimpleNamespace(**dict(zip(names, refs)))


def taker(refs):
    refs = list(refs)

    def take(number):
        head = refs[:number]
        del refs[:number]
        return head

    return take


def first_kernel(chips, early, parts, late_parts, *refs):
    take = taker(refs)
    late = LATE
    g, late_g, w, late_w = take(early), take(late), take(early), take(late)
    m, late_m, v, late_v = take(early), take(late), take(early), take(late)
    w_out, m_out, v_out = (take(early) for _ in range(3))
    held, new_w, new_m, new_v = (take(late) for _ in range(4))
    own, wb = take(early), take(early)
    late_own, late_wb, work, work_m, work_v = (take(late) for _ in range(5))
    sems, late_sems = (named(names, take(len(names))) for names in (GIVE + RING + GATHER, KEPT + RING))
    hold_send, hold_recv, store = take(3)
    at = place(chips)
    last = at.last
    a = engine(at, parts, g, w_out, m_out, v_out, own, wb, sems)
    b = engine(at, late_parts, late_g, work, work_m, work_v, late_own, late_wb, late_sems, held)

    def hold(s, k, d):
        half, rows = held[k].shape[2:4]
        where = pl.ds(pl.multiple_of((at.turn(d, s) * CORES + at.other) * rows, rows), rows)
        return pltpu.make_async_remote_copy(
            late_g[k].at[0, pl.ds(d * half, half), where],
            held[k].at[s, d],
            hold_send.at[k],
            hold_recv.at[s, k],
            device_id=at.partner,
        )

    pairs = [(k, d) for k in range(late) for d in range(WAYS)]

    def kept(s):
        for k in range(late):
            b.wait_all(held[k].at[s], hold_recv.at[s, k])

    def store_new(p):
        k, d, _, _ = late_parts[p]
        rows = b.within(p)
        return [
            pltpu.make_async_copy(b.slot(p, at.z, at.c), new_w[k].at[d, :, rows], store.at[0, k]),
            pltpu.make_async_copy(work_m[k].at[b.layers(p), rows], new_m[k].at[b.layers(p), rows], store.at[1, k]),
            pltpu.make_async_copy(work_v[k].at[b.layers(p), rows], new_v[k].at[b.layers(p), rows], store.at[2, k]),
        ]

    barrier = pltpu.get_barrier_semaphore()
    for device in (*at.ahead, at.partner):
        pl.semaphore_signal(barrier, inc=1, device_id=device)
    for s in range(2):
        for k in range(early):
            a.load_own(s, k)
    pl.semaphore_wait(barrier, 3)
    for p in a.parts:
        a.give(0, p).start()
    for k in range(early):
        a.give_all(1, k)
    for p in a.parts:
        a.add(0, p, True)
    for k in range(early):
        a.fetch(2, k)
        a.load_state(k, w, m, v)
    a.reduce_middle(1)
    for p in a.parts:
        a.add(last - 1, p)
        a.may_land(0, p)
    for p in a.parts:
        a.update(p)
        a.gather_after(0, 0, p)
        a.may_side(p)
        if p:
            a.first_side(p - 1)
    a.first_side(len(parts) - 1)
    for p in a.parts:
        a.ring(last - 1, p).wait_send()
        a.may_land(1, p)

    @pl.loop(1, last - 1)
    def _(t):
        for p in a.parts:
            a.onward(t, p)
        for k, d in pairs:
            hold(t - 1, k, d).start()

    for s in range(last - 2, chips):
        for k, d in pairs:
            hold(s, k, d).start()
    for p in a.parts:
        a.onward(last - 1, p, 1)

    @pl.when(at.c == 1)
    def _():
        for s in range(2):
            kept(s)
            for k in range(late):
                b.fetch(s, k)
        for p in b.parts:
            b.add(0, p, True)
        kept(2)
        for k in range(late):
            b.fetch(2, k)

    for p in a.parts:
        a.gather(last - 1, p).wait_recv()
        a.side(last, p).start()

    @pl.loop(3, chips)
    def _(s):
        kept(s)

    @pl.when(at.c == 1)
    def _():
        for k in range(late):
            b.load_state(k, late_w, late_m, late_v)
        b.reduce_middle(1)
        for p in b.parts:
            b.add(last - 1, p)
        for p in b.parts:
            b.update(p)
            for copy in store_new(p):
                copy.start()
        for p in b.parts:
            b.ring(last - 1, p).wait_send()
        for k in range(late):
            for i, ref in enumerate((new_w, new_m, new_v)):
                b.wait_all(ref[k], store.at[i, k])

    @pl.when(at.c == 0)
    def _():
        for s in range(3):
            kept(s)

    a.end_give()
    a.end_gather()
    for k in range(late):
        b.wait_all(held[k], hold_send.at[k])


def second_kernel(chips, parts, *refs):
    take = taker(refs)
    count = LATE
    g, w, m, v, held, new_w, new_m, new_v = (take(count) for _ in range(8))
    take(1)
    w_out, m_out, v_out = (take(count) for _ in range(3))
    own, wb = take(count), take(count)
    sems = named(KEPT + RING + GATHER, take(len(KEPT + RING + GATHER)))
    at = place(chips)
    last = at.last
    a = engine(at, parts, g, w_out, m_out, v_out, own, wb, sems, held)

    def bring(k):
        for d in range(WAYS):
            here = w_out[k].at[a.all_of(k, d, at.z, at.c)]
            pltpu.make_async_copy(new_w[k].at[d], here, sems.state.at[0, k]).start()
        pltpu.make_async_copy(new_m[k], m_out[k], sems.state.at[1, k]).start()
        pltpu.make_async_copy(new_v[k], v_out[k], sems.state.at[2, k]).start()

    barrier = pltpu.get_barrier_semaphore()
    for device in at.ahead:
        pl.semaphore_signal(barrier, inc=1, device_id=device)

    @pl.when(at.c == 0)
    def _():
        for s in range(2):
            for k in range(count):
                a.fetch(s, k)
        pl.semaphore_wait(barrier, 2)
        pl.semaphore_signal(barrier, inc=1, device_id=at.partner)
        for p in a.parts:
            a.add(0, p, True)
        for k in range(count):
            a.fetch(2, k)
            a.load_state(k, w, m, v)
        a.reduce_middle(1)
        for p in a.parts:
            a.add(last - 1, p)
            a.may_land(0, p)
        for p in a.parts:
            a.update(p)
            a.gather_after(0, 0, p)
        for p in a.parts:
            a.ring(last - 1, p).wait_send()
            a.may_land(1, p)
        pl.semaphore_wait(barrier, 1)

    @pl.when(at.c == 1)
    def _():
        for k in range(count):
            bring(k)
        pl.semaphore_wait(barrier, 3)
        pl.semaphore_signal(barrier, inc=1, device_id=at.partner)
        for p in a.parts:
            for which in range(2):
                a.may_land(which, p)
        for k in range(count):
            for i, ref in enumerate((new_w, m_out, v_out)):
                a.wait_all(ref[k], sems.state.at[i, k])
        for p in a.parts:
            a.gather_after(0, 0, p)

    for p in a.parts:
        a.may_side(p)
    for p in a.parts:
        a.first_side(p)

    @pl.loop(1, last - 1)
    def _(t):
        for p in a.parts:
            a.onward(t, p)

    for p in a.parts:
        a.onward(last - 1, p, 1)
    for p in a.parts:
        a.gather(last - 1, p).wait_recv()
        a.side(last, p).start()
    a.end_gather()


def settle(count, *refs):
    sources, targets, sem = refs[:count], refs[count : 2 * count], refs[-1]
    copies = [
        pltpu.make_async_copy(source.at[layer], target.at[layer], sem.at[i, layer])
        for i, (source, target) in enumerate(zip(sources, targets))
        for layer in range(source.shape[0])
    ]
    for copy in copies:
        copy.start()
    for copy in copies:
        copy.wait()


def solution(mesh):
    chips = mesh.shape["dp"] // CORES
    any_of, vmem = (pl.BlockSpec(memory_space=space) for space in (pl.ANY, pltpu.VMEM))
    dma = pltpu.SemaphoreType.DMA
    mib = 1024 * 1024

    def in_hbm(arrays):
        return [pltpu.with_memory_space_constraint(one, pltpu.HBM) for one in arrays]

    def out(arrays):
        layers = max(one.shape[0] for one in arrays)
        shapes = [jax.ShapeDtypeStruct(one.shape, one.dtype) for one in arrays]
        return pl.pallas_call(
            functools.partial(settle, len(arrays)),
            out_shape=shapes,
            in_specs=[vmem] * len(arrays),
            out_specs=[any_of] * len(arrays),
            scratch_shapes=[dma((len(arrays), layers))],
            compiler_params=pltpu.CompilerParams(vmem_limit_bytes=2 * mib),
        )(*(pltpu.with_memory_space_constraint(one, pltpu.VMEM) for one in arrays))

    def step(*arrays):
        terms, weights, m, v = (arrays[i : i + 3] for i in (0, 3, 6, 9))
        early = len(weights) - LATE
        shapes = [(one.shape[0] // WAYS, *one.shape[1:]) for one in m]
        parts, late_parts = parts_of(m[:early], [FIRST] + [(1,)] * (early - 1)), parts_of(m[early:], [PIECES] * LATE)

        def slots(some, number, dtype=jnp.bfloat16):
            return [pltpu.VMEM((*number, *one), dtype) for one in some]

        late_shapes = shapes[early:]
        results = pl.pallas_call(
            functools.partial(first_kernel, chips, early, parts, late_parts),
            out_shape=[
                *(pltpu.VMEM(one.shape, one.dtype) for one in (*weights[:early], *m[:early], *v[:early])),
                *(pltpu.HBM((chips, WAYS, *one), jnp.bfloat16) for one in late_shapes),
                *(pltpu.HBM((WAYS, *one), jnp.bfloat16) for one in late_shapes),
                *(pltpu.HBM(one.shape, one.dtype) for one in (*m[early:], *v[early:])),
            ],
            in_specs=[any_of] * len(arrays),
            out_specs=[vmem] * (3 * early) + [any_of] * (4 * LATE),
            scratch_shapes=[
                *slots(shapes[:early], (2, WAYS)),
                *slots(shapes[:early], (WAYS,)),
                *slots(late_shapes, (2, WAYS)),
                *slots(late_shapes, (WAYS,)),
                *(pltpu.VMEM(one.shape, one.dtype) for one in (*weights[early:], *m[early:], *v[early:])),
                *semaphores(chips, len(parts), early, GIVE + RING + GATHER),
                *semaphores(chips, len(late_parts), LATE, KEPT + RING),
                dma((LATE,)),
                dma((chips, LATE)),
                dma((3, LATE)),
            ],
            compiler_params=pltpu.CompilerParams(collective_id=0, has_side_effects=True, vmem_limit_bytes=24 * mib),
        )(*in_hbm(arrays))
        (w1, m1, v1), rest = (results[i : i + early] for i in (0, early, 2 * early)), results[3 * early :]
        done = out([*w1, *m1, *v1])
        late = [one for kind in (terms, weights, m, v) for one in kind[early:]]
        results = pl.pallas_call(
            functools.partial(second_kernel, chips, late_parts),
            out_shape=[pltpu.VMEM(one.shape, one.dtype) for one in (*weights[early:], *m[early:], *v[early:])],
            in_specs=[any_of] * (len(late) + len(rest) + 1),
            out_specs=[vmem] * (3 * LATE),
            scratch_shapes=[
                *slots(late_shapes, (2, WAYS)),
                *slots(late_shapes, (WAYS,)),
                *semaphores(chips, len(late_parts), LATE, KEPT + RING + GATHER),
            ],
            compiler_params=pltpu.CompilerParams(collective_id=1, has_side_effects=True, vmem_limit_bytes=8 * mib),
        )(*in_hbm([*late, *rest, done[-1]]))
        then = out(results)
        return tuple(
            one
            for i in range(3)
            for one in (*done[i * early : (i + 1) * early], *then[i * LATE : (i + 1) * LATE])
        )

    all_of, sharded = P(None, None, None), P(None, "dp", None)
    return jax.shard_map(
        step,
        mesh=mesh,
        in_specs=(P(("rep", "dp"), None, None, None),) * 3 + (all_of,) * 3 + (sharded,) * 6,
        out_specs=(P("rep", None, None),) * 3 + (P("rep", "dp", None),) * 6,
        check_vma=False,
    )
```

```python
import functools
import types

import jax
import jax.numpy as jnp
from jax import lax
from jax.experimental import pallas as pl
from jax.experimental.pallas import tpu as pltpu
from jax.sharding import PartitionSpec as P

CORES = 2
ROWS = 16
WAYS = 2
LATE = 1
FIRST = (1, 3)
PIECES = (3, 3, 3, 2)


def adamw(w, m, v, g):
    m = 0.9 * m + 0.1 * g
    v = 0.95 * v + 0.05 * g * g
    step = m * lax.rsqrt(v + 1e-8) + 0.1 * w
    return (w - 0.02 * step).astype(jnp.bfloat16), m, v


def cut(rows, shares):
    tiles = rows // ROWS
    ends = [tiles * sum(shares[:i]) // sum(shares) * ROWS for i in range(len(shares) + 1)]
    return [(a, b - a) for a, b in zip(ends, ends[1:]) if b > a]


def parts_of(state, shares):
    return [
        (k, d, *piece)
        for k, (one, some) in enumerate(zip(state, shares))
        for piece in cut(one.shape[-2], some)
        for d in range(WAYS)
    ]


def place(chips):
    me = lax.axis_index("dp")
    z, c = me // CORES, me % CORES

    def chip(i):
        return (i + 2 * chips) % chips

    ahead = [{"dp": chip(z + 1) * CORES + c}, {"dp": chip(z - 1) * CORES + c}]
    return types.SimpleNamespace(
        chips=chips,
        last=chips - 1,
        z=z,
        c=c,
        other=1 - c,
        chip=chip,
        partner={"dp": z * CORES + 1 - c},
        ahead=ahead,
        behind=ahead[::-1],
        turn=lambda d, s: chip(z - 1 - s) if d == 0 else chip(z + 1 + s),
    )


def engine(at, parts, g, w_out, m_out, v_out, own, wb, sems, held=None):
    e = types.SimpleNamespace(parts=range(len(parts)))
    half = [one.shape[0] // WAYS for one in m_out]
    block_rows = [one.shape[1] for one in m_out]

    def layers(p):
        k, d, _, _ = parts[p]
        return pl.ds(d * half[k], half[k])

    def within(p):
        return pl.ds(parts[p][2], parts[p][3])

    def rows_of(p, chip_of, core):
        k, _, start, size = parts[p]
        return pl.ds(pl.multiple_of((chip_of * CORES + core) * block_rows[k] + start, ROWS), size)

    def slot(p, chip_of, core):
        return w_out[parts[p][0]].at[layers(p), rows_of(p, chip_of, core)]

    ways = range(WAYS)
    opens = [all(parts[q][0] != part[0] for q in range(p)) for p, part in enumerate(parts)]
    closes = [all(parts[q][0] != part[0] for q in range(p + 1, len(parts))) for p, part in enumerate(parts)]

    def all_of(k, d, chip_of, core):
        start = pl.multiple_of((chip_of * CORES + core) * block_rows[k], block_rows[k])
        return pl.ds(d * half[k], half[k]), pl.ds(start, block_rows[k])

    def blocks(k, number):
        return w_out[k].at[:, pl.ds(0, number * block_rows[k])]

    def wait_all(ref, sem):
        pltpu.make_async_copy(ref, ref, sem).wait()

    def load_own(s, k):
        for d in ways:
            here = (0, *all_of(k, d, at.turn(d, s), at.c))
            pltpu.make_async_copy(g[k].at[here], own[k].at[s % 2, d], sems.own.at[s % 2, k]).start()

    def give(s, p):
        k, d, _, _ = parts[p]
        where = rows_of(p, at.turn(d, s), at.other)
        return pltpu.make_async_remote_copy(
            g[k].at[0, layers(p), where],
            w_out[k].at[layers(p), where],
            sems.give_send.at[k],
            sems.first_recv.at[p],
            device_id=at.partner,
        )

    def give_all(s, k):
        for d in ways:
            if held is not None:
                slot_of = w_out[k].at[all_of(k, d, at.turn(d, s), at.c)]
                pltpu.make_async_copy(held[k].at[s, d], slot_of, sems.kept.at[s % 2, k]).start()
            else:
                where = all_of(k, d, at.turn(d, s), at.other)
                pltpu.make_async_remote_copy(
                    g[k].at[(0, *where)],
                    w_out[k].at[where],
                    sems.give_send.at[k],
                    sems.give_recv.at[s, k],
                    device_id=at.partner,
                ).start()

    def ring(s, p):
        d = parts[p][1]
        return pltpu.make_async_remote_copy(
            slot(p, at.turn(d, s), at.c),
            slot(p, at.turn(d, s), at.other),
            sems.ring_send.at[s % 2, p],
            sems.ring_recv.at[s, p],
            device_id=at.ahead[d],
        )

    def travelling(t, p):
        return slot(p, at.chip(at.z - t) if parts[p][1] == 0 else at.chip(at.z + t), at.c)

    def gather(t, p):
        here = travelling(t, p)
        return pltpu.make_async_remote_copy(
            here, here, sems.ag_send.at[parts[p][0]], sems.ring_recv.at[t, p], device_id=at.ahead[parts[p][1]]
        )

    def side(t, p):
        here = travelling(t, p)
        k = parts[p][0]
        return pltpu.make_async_remote_copy(here, here, sems.side_send.at[k], sems.side_recv.at[k], device_id=at.partner)

    def by_rows(p, body):
        for h in range(half[parts[p][0]]):

            @pl.loop(0, parts[p][3] // ROWS)
            def _(i):
                body(h, i * ROWS)

    def tile(p, chip_of, core, h, row):
        k, d, start, _ = parts[p]
        first = pl.multiple_of((chip_of * CORES + core) * block_rows[k] + start + row, ROWS)
        return d * half[k] + h, pl.ds(first, ROWS)

    def total(s, p, h, row, first):
        k, d, start, _ = parts[p]
        mine = own[k][s % 2, d, h, pl.ds(pl.multiple_of(start + row, ROWS), ROWS)]
        so_far = mine.astype(jnp.float32) + w_out[k][tile(p, at.turn(d, s), at.c, h, row)].astype(jnp.float32)
        if not first:
            so_far = so_far + w_out[k][tile(p, at.turn(d, s), at.other, h, row)].astype(jnp.float32)
        return so_far.astype(jnp.bfloat16)

    def fetch(s, k):
        load_own(s, k)
        give_all(s, k)

    def arrive(s, p, first):
        k = parts[p][0]
        if opens[p]:
            wait_all(own[k].at[s % 2], sems.own.at[s % 2, k])
            if held is not None:
                wait_all(blocks(k, 1), sems.kept.at[s % 2, k])
            elif not first:
                wait_all(blocks(k, 1), sems.give_recv.at[s, k])
        if first and held is None:
            give(s, p).wait_recv()
        if not first:
            ring(s - 1, p).wait_recv()

    def add(s, p, first=False, then=None):
        arrive(s, p, first)
        if then is not None:
            then()

        def body(h, row):
            k, d, _, _ = parts[p]
            w_out[k][tile(p, at.turn(d, s), at.c, h, row)] = total(s, p, h, row, first)

        by_rows(p, body)
        ring(s, p).start()
        if not first:
            ring(s - 1, p).wait_send()

    def load_state(k, w, m, v):
        for d in ways:
            here = all_of(k, d, at.z, at.c)
            pltpu.make_async_copy(w[k].at[here], wb[k].at[d], sems.state.at[0, k]).start()
        pltpu.make_async_copy(m[k], m_out[k], sems.state.at[1, k]).start()
        pltpu.make_async_copy(v[k], v_out[k], sems.state.at[2, k]).start()

    def update(p):
        arrive(at.last, p, False)
        if opens[p]:
            for i, ref in enumerate((wb, m_out, v_out)):
                wait_all(ref[parts[p][0]], sems.state.at[i, parts[p][0]])

        def body(h, row):
            k, d, start, _ = parts[p]
            grad = total(at.last, p, h, row, False).astype(jnp.float32)
            here = pl.ds(pl.multiple_of(start + row, ROWS), ROWS)
            state = d * half[k] + h, here
            old = wb[k][d, h, here].astype(jnp.float32)
            new = adamw(old, m_out[k][state], v_out[k][state], grad)
            w_out[k][tile(p, at.z, at.c, h, row)], m_out[k][state], v_out[k][state] = new

        by_rows(p, body)

    def reduce_middle(first_step):
        @pl.loop(first_step, at.last - 1)
        def _(s):
            for p in e.parts:
                add(s, p)
                if closes[p]:
                    fetch(s + 2, parts[p][0])

    def may_land(which, p):
        pl.semaphore_signal(sems.clear.at[which, p], inc=1, device_id=at.behind[parts[p][1]])

    def gather_after(which, t, p):
        pl.semaphore_wait(sems.clear.at[which, p], 1)
        gather(t, p).start()

    def may_side(p):
        if closes[p]:
            pl.semaphore_signal(sems.free.at[parts[p][0]], inc=1, device_id=at.partner)

    def first_side(p):
        if opens[p]:
            pl.semaphore_wait(sems.free.at[parts[p][0]], 1)
        side(0, p).start()

    def onward(t, p, which=None):
        gather(t - 1, p).wait_recv()
        if which is None:
            gather(t, p).start()
        else:
            gather_after(which, t, p)
        side(t, p).start()

    def end_gather():
        for k in range(len(w_out)):
            wait_all(blocks(k, at.last), sems.ag_send.at[k])
            wait_all(blocks(k, at.chips), sems.side_send.at[k])
            wait_all(blocks(k, at.chips), sems.side_recv.at[k])

    def end_give():
        for k in range(len(w_out)):
            wait_all(blocks(k, at.chips), sems.give_send.at[k])

    for one in (
        fetch, load_own, give, give_all, add, load_state, wait_all, all_of, update, reduce_middle, may_land, gather_after, may_side, first_side, onward, end_gather, end_give,
        ring, gather, side, slot, layers, within,
    ):
        setattr(e, one.__name__, one)
    return e


GIVE = ("first_recv", "give_send", "give_recv")
KEPT = ("kept",)
RING = ("own", "ring_send", "ring_recv", "state")
GATHER = ("ag_send", "side_send", "side_recv", "free", "clear")


def semaphores(chips, count, weights, names):
    dma, plain = pltpu.SemaphoreType.DMA, pltpu.SemaphoreType.REGULAR
    shape = dict(
        first_recv=dma((count,)), give_send=dma((weights,)), give_recv=dma((chips, weights)),
        kept=dma((2, weights)), own=dma((2, weights)), ring_send=dma((2, count)), ring_recv=dma((chips - 1, count)),
        state=dma((3, weights)), ag_send=dma((weights,)), side_send=dma((weights,)),
        side_recv=dma((weights,)), free=plain((weights,)), clear=plain((2, count)),
    )
    return [shape[name] for name in names]


def named(names, refs):
    return types.SimpleNamespace(**dict(zip(names, refs)))


def taker(refs):
    refs = list(refs)

    def take(number):
        head = refs[:number]
        del refs[:number]
        return head

    return take


def first_kernel(chips, early, parts, late_parts, *refs):
    take = taker(refs)
    late = LATE
    g, late_g, w, late_w = take(early), take(late), take(early), take(late)
    m, late_m, v, late_v = take(early), take(late), take(early), take(late)
    w_out, m_out, v_out = (take(early) for _ in range(3))
    held, new_w, new_m, new_v = (take(late) for _ in range(4))
    own, wb = take(early), take(early)
    late_own, late_wb, work, work_m, work_v = (take(late) for _ in range(5))
    sems, late_sems = (named(names, take(len(names))) for names in (GIVE + RING + GATHER, KEPT + RING))
    hold_send, hold_recv, store = take(3)
    at = place(chips)
    last = at.last
    a = engine(at, parts, g, w_out, m_out, v_out, own, wb, sems)
    b = engine(at, late_parts, late_g, work, work_m, work_v, late_own, late_wb, late_sems, held)

    def hold(s, k, d):
        half, rows = held[k].shape[2:4]
        where = pl.ds(pl.multiple_of((at.turn(d, s) * CORES + at.other) * rows, rows), rows)
        return pltpu.make_async_remote_copy(
            late_g[k].at[0, pl.ds(d * half, half), where],
            held[k].at[s, d],
            hold_send.at[k],
            hold_recv.at[s, k],
            device_id=at.partner,
        )

    pairs = [(k, d) for k in range(late) for d in range(WAYS)]

    def kept(s):
        for k in range(late):
            b.wait_all(held[k].at[s], hold_recv.at[s, k])

    def store_new(p):
        k, d, _, _ = late_parts[p]
        rows = b.within(p)
        return [
            pltpu.make_async_copy(b.slot(p, at.z, at.c), new_w[k].at[d, :, rows], store.at[0, k]),
            pltpu.make_async_copy(work_m[k].at[b.layers(p), rows], new_m[k].at[b.layers(p), rows], store.at[1, k]),
            pltpu.make_async_copy(work_v[k].at[b.layers(p), rows], new_v[k].at[b.layers(p), rows], store.at[2, k]),
        ]

    barrier = pltpu.get_barrier_semaphore()
    for device in (*at.ahead, at.partner):
        pl.semaphore_signal(barrier, inc=1, device_id=device)
    for s in range(2):
        for k in range(early):
            a.load_own(s, k)
    pl.semaphore_wait(barrier, 3)
    for p in a.parts:
        a.give(0, p).start()
    for k in range(early):
        a.give_all(1, k)
    for p in a.parts:
        a.add(0, p, True)
    for k in range(early):
        a.fetch(2, k)
        a.load_state(k, w, m, v)
    a.reduce_middle(1)
    for p in a.parts:
        a.add(last - 1, p)
        a.may_land(0, p)
    for p in a.parts:
        a.update(p)
        a.gather_after(0, 0, p)
        a.may_side(p)
    for p in a.parts:
        a.first_side(p)
    for p in a.parts:
        a.ring(last - 1, p).wait_send()
        a.may_land(1, p)

    @pl.loop(1, last - 1)
    def _(t):
        for p in a.parts:
            a.onward(t, p)
        for k, d in pairs:
            hold(t - 1, k, d).start()

    for s in range(last - 2, chips):
        for k, d in pairs:
            hold(s, k, d).start()
    for p in a.parts:
        a.onward(last - 1, p, 1)

    @pl.when(at.c == 1)
    def _():
        for s in range(2):
            kept(s)
            for k in range(late):
                b.fetch(s, k)
        for p in b.parts:
            b.add(0, p, True)
        kept(2)
        for k in range(late):
            b.fetch(2, k)

    for p in a.parts:
        a.gather(last - 1, p).wait_recv()
        a.side(last, p).start()

    @pl.loop(3, chips)
    def _(s):
        kept(s)

    @pl.when(at.c == 1)
    def _():
        for k in range(late):
            b.load_state(k, late_w, late_m, late_v)
        b.reduce_middle(1)
        for p in b.parts:
            b.add(last - 1, p)
        for p in b.parts:
            b.update(p)
            for copy in store_new(p):
                copy.start()
        for p in b.parts:
            b.ring(last - 1, p).wait_send()
        for k in range(late):
            for i, ref in enumerate((new_w, new_m, new_v)):
                b.wait_all(ref[k], store.at[i, k])

    @pl.when(at.c == 0)
    def _():
        for s in range(3):
            kept(s)

    a.end_give()
    a.end_gather()
    for k in range(late):
        b.wait_all(held[k], hold_send.at[k])


def second_kernel(chips, parts, *refs):
    take = taker(refs)
    count = LATE
    g, w, m, v, held, new_w, new_m, new_v = (take(count) for _ in range(8))
    take(1)
    w_out, m_out, v_out = (take(count) for _ in range(3))
    own, wb = take(count), take(count)
    sems = named(KEPT + RING + GATHER, take(len(KEPT + RING + GATHER)))
    at = place(chips)
    last = at.last
    a = engine(at, parts, g, w_out, m_out, v_out, own, wb, sems, held)

    def bring(k):
        for d in range(WAYS):
            here = w_out[k].at[a.all_of(k, d, at.z, at.c)]
            pltpu.make_async_copy(new_w[k].at[d], here, sems.state.at[0, k]).start()
        pltpu.make_async_copy(new_m[k], m_out[k], sems.state.at[1, k]).start()
        pltpu.make_async_copy(new_v[k], v_out[k], sems.state.at[2, k]).start()

    barrier = pltpu.get_barrier_semaphore()
    for device in at.ahead:
        pl.semaphore_signal(barrier, inc=1, device_id=device)

    @pl.when(at.c == 0)
    def _():
        for s in range(2):
            for k in range(count):
                a.fetch(s, k)
        pl.semaphore_wait(barrier, 2)
        pl.semaphore_signal(barrier, inc=1, device_id=at.partner)
        for p in a.parts:
            a.add(0, p, True)
        for k in range(count):
            a.fetch(2, k)
            a.load_state(k, w, m, v)
        a.reduce_middle(1)
        for p in a.parts:
            a.add(last - 1, p)
            a.may_land(0, p)
        for p in a.parts:
            a.update(p)
            a.gather_after(0, 0, p)
        for p in a.parts:
            a.ring(last - 1, p).wait_send()
            a.may_land(1, p)
        pl.semaphore_wait(barrier, 1)

    @pl.when(at.c == 1)
    def _():
        for k in range(count):
            bring(k)
        pl.semaphore_wait(barrier, 3)
        pl.semaphore_signal(barrier, inc=1, device_id=at.partner)
        for p in a.parts:
            for which in range(2):
                a.may_land(which, p)
        for k in range(count):
            for i, ref in enumerate((new_w, m_out, v_out)):
                a.wait_all(ref[k], sems.state.at[i, k])
        for p in a.parts:
            a.gather_after(0, 0, p)

    for p in a.parts:
        a.may_side(p)
    for p in a.parts:
        a.first_side(p)

    @pl.loop(1, last - 1)
    def _(t):
        for p in a.parts:
            a.onward(t, p)

    for p in a.parts:
        a.onward(last - 1, p, 1)
    for p in a.parts:
        a.gather(last - 1, p).wait_recv()
        a.side(last, p).start()
    a.end_gather()


def settle(count, *refs):
    sources, targets, sem = refs[:count], refs[count : 2 * count], refs[-1]
    copies = [
        pltpu.make_async_copy(source.at[layer], target.at[layer], sem.at[i, layer])
        for i, (source, target) in enumerate(zip(sources, targets))
        for layer in range(source.shape[0])
    ]
    for copy in copies:
        copy.start()
    for copy in copies:
        copy.wait()


def solution(mesh):
    chips = mesh.shape["dp"] // CORES
    any_of, vmem = (pl.BlockSpec(memory_space=space) for space in (pl.ANY, pltpu.VMEM))
    dma = pltpu.SemaphoreType.DMA
    mib = 1024 * 1024

    def in_hbm(arrays):
        return [pltpu.with_memory_space_constraint(one, pltpu.HBM) for one in arrays]

    def out(arrays):
        layers = max(one.shape[0] for one in arrays)
        shapes = [jax.ShapeDtypeStruct(one.shape, one.dtype) for one in arrays]
        return pl.pallas_call(
            functools.partial(settle, len(arrays)),
            out_shape=shapes,
            in_specs=[vmem] * len(arrays),
            out_specs=[any_of] * len(arrays),
            scratch_shapes=[dma((len(arrays), layers))],
            compiler_params=pltpu.CompilerParams(vmem_limit_bytes=2 * mib),
        )(*(pltpu.with_memory_space_constraint(one, pltpu.VMEM) for one in arrays))

    def step(*arrays):
        terms, weights, m, v = (arrays[i : i + 3] for i in (0, 3, 6, 9))
        early = len(weights) - LATE
        shapes = [(one.shape[0] // WAYS, *one.shape[1:]) for one in m]
        parts, late_parts = parts_of(m[:early], [FIRST] + [(1,)] * (early - 1)), parts_of(m[early:], [PIECES] * LATE)

        def slots(some, number, dtype=jnp.bfloat16):
            return [pltpu.VMEM((*number, *one), dtype) for one in some]

        late_shapes = shapes[early:]
        results = pl.pallas_call(
            functools.partial(first_kernel, chips, early, parts, late_parts),
            out_shape=[
                *(pltpu.VMEM(one.shape, one.dtype) for one in (*weights[:early], *m[:early], *v[:early])),
                *(pltpu.HBM((chips, WAYS, *one), jnp.bfloat16) for one in late_shapes),
                *(pltpu.HBM((WAYS, *one), jnp.bfloat16) for one in late_shapes),
                *(pltpu.HBM(one.shape, one.dtype) for one in (*m[early:], *v[early:])),
            ],
            in_specs=[any_of] * len(arrays),
            out_specs=[vmem] * (3 * early) + [any_of] * (4 * LATE),
            scratch_shapes=[
                *slots(shapes[:early], (2, WAYS)),
                *slots(shapes[:early], (WAYS,)),
                *slots(late_shapes, (2, WAYS)),
                *slots(late_shapes, (WAYS,)),
                *(pltpu.VMEM(one.shape, one.dtype) for one in (*weights[early:], *m[early:], *v[early:])),
                *semaphores(chips, len(parts), early, GIVE + RING + GATHER),
                *semaphores(chips, len(late_parts), LATE, KEPT + RING),
                dma((LATE,)),
                dma((chips, LATE)),
                dma((3, LATE)),
            ],
            compiler_params=pltpu.CompilerParams(collective_id=0, has_side_effects=True, vmem_limit_bytes=24 * mib),
        )(*in_hbm(arrays))
        (w1, m1, v1), rest = (results[i : i + early] for i in (0, early, 2 * early)), results[3 * early :]
        done = out([*w1, *m1, *v1])
        late = [one for kind in (terms, weights, m, v) for one in kind[early:]]
        results = pl.pallas_call(
            functools.partial(second_kernel, chips, late_parts),
            out_shape=[pltpu.VMEM(one.shape, one.dtype) for one in (*weights[early:], *m[early:], *v[early:])],
            in_specs=[any_of] * (len(late) + len(rest) + 1),
            out_specs=[vmem] * (3 * LATE),
            scratch_shapes=[
                *slots(late_shapes, (2, WAYS)),
                *slots(late_shapes, (WAYS,)),
                *semaphores(chips, len(late_parts), LATE, KEPT + RING + GATHER),
            ],
            compiler_params=pltpu.CompilerParams(collective_id=1, has_side_effects=True, vmem_limit_bytes=8 * mib),
        )(*in_hbm([*late, *rest, done[-1]]))
        then = out(results)
        return tuple(
            one
            for i in range(3)
            for one in (*done[i * early : (i + 1) * early], *then[i * LATE : (i + 1) * LATE])
        )

    all_of, sharded = P(None, None, None), P(None, "dp", None)
    return jax.shard_map(
        step,
        mesh=mesh,
        in_specs=(P(("rep", "dp"), None, None, None),) * 3 + (all_of,) * 3 + (sharded,) * 6,
        out_specs=(P("rep", None, None),) * 3 + (P("rep", "dp", None),) * 6,
        check_vma=False,
    )
```
